8 devices in a mesh: dp: 1 (over z), sp: 8 (over y, x, core).
Axes of the slice: x: 2, y: 2, z: 1, core: 2. Of those that a mesh axis runs over, the one named last changes fastest.
Arguments:
- hidden: bfloat16 [8, 1024, 2048], P('dp', 'sp')
- norm_w: bfloat16 [2048], replicated
- w_qkv: bfloat16 [2048, 3072], replicated
- w_out: bfloat16 [32, 64, 2048], replicated
- long_factor: float32 [32], replicated
- grad_out: bfloat16 [8, 1024, 2048], P('dp', 'sp')
Outputs:
- output 1: bfloat16 [8, 1024, 2048], P('dp', 'sp')
- output 2: bfloat16 [8, 1024, 2048], P('dp', 'sp')
- output 3: float32 [2048, 3072], P('dp')
- output 4: float32 [32, 64, 2048], P('dp')
- output 5: float32 [2048], P('dp')
All inputs are finite; a program needn't handle non-finite values.
Results may differ from the reference program's by a relative error of at most 0.0104923.
Values are sent between devices in bfloat16 or wider.
A program may use at most 1 GiB of HBM per device.

```python
import math
import jax
import jax.numpy as jnp
from jax import lax

N_BATCH = 8
SEQ_LEN = 1024
D_MODEL = 2048
N_HEADS = 32
N_KV_HEADS = 8
HEAD_DIM = 64
ROT_DIM = 64

Q_WIDTH = N_HEADS * HEAD_DIM
KV_WIDTH = N_KV_HEADS * HEAD_DIM
QKV_WIDTH = Q_WIDTH + 2 * KV_WIDTH
GROUP_SIZE = N_HEADS // N_KV_HEADS
HALF_ROT = ROT_DIM // 2
NORM_EPS = 1e-5
ROPE_BASE = 10000.0
ROPE_GAIN = math.sqrt(1.0 + math.log(32.0) / math.log(4096.0))
MASK_VALUE = -1e30


def setup_inputs(seed: int = 0, part: int = 0) -> dict:
    part_key = jax.random.fold_in(jax.random.key(seed), part)
    key_hidden, key_grad = jax.random.split(part_key, 2)
    key_norm, key_qkv, key_out, key_factor = jax.random.split(jax.random.key(seed + 1), 4)
    act_shape = (N_BATCH, SEQ_LEN, D_MODEL)
    hidden = jax.random.normal(key_hidden, act_shape, jnp.float32)
    grad_out = jax.random.normal(key_grad, act_shape, jnp.float32)
    norm_w = jax.random.uniform(key_norm, (D_MODEL,), jnp.float32, 0.5, 1.5)
    w_qkv = jax.random.normal(key_qkv, (D_MODEL, QKV_WIDTH), jnp.float32) * (D_MODEL ** -0.5)
    out_std = (SEQ_LEN / (64.0 * Q_WIDTH)) ** 0.5
    w_out = jax.random.normal(key_out, (N_HEADS, HEAD_DIM, D_MODEL), jnp.float32) * out_std
    long_factor = jnp.exp(jax.random.uniform(key_factor, (HALF_ROT,), jnp.float32, 0.0, math.log(48.0)))
    return {
        'hidden': hidden.astype(jnp.bfloat16),
        'norm_w': norm_w.astype(jnp.bfloat16),
        'w_qkv': w_qkv.astype(jnp.bfloat16),
        'w_out': w_out.astype(jnp.bfloat16),
        'long_factor': long_factor,
        'grad_out': grad_out.astype(jnp.bfloat16),
    }


def to_grid(values):
    return values.astype(jnp.bfloat16).astype(jnp.float32)


def rope_tables(long_factor):
    positions = jnp.arange(SEQ_LEN).astype(jnp.float32)
    exponent = jnp.arange(HALF_ROT).astype(jnp.float32) / HALF_ROT
    inv_freq = 1.0 / (long_factor.astype(jnp.float32) * jnp.power(ROPE_BASE, exponent))
    angles = positions[:, None] * inv_freq[None, :]
    return jnp.cos(angles) * ROPE_GAIN, jnp.sin(angles) * ROPE_GAIN


def rotate(head_vals, cos_t, sin_t):
    cos_b = cos_t[None, :, None, :]
    sin_b = sin_t[None, :, None, :]
    first_half = head_vals[..., :HALF_ROT]
    second_half = head_vals[..., HALF_ROT:ROT_DIM]
    return jnp.concatenate([first_half * cos_b - second_half * sin_b, second_half * cos_b + first_half * sin_b, head_vals[..., ROT_DIM:]], axis=-1)


def head_attention(q_head, k_head, v_head):
    causal = jnp.arange(SEQ_LEN)[:, None] >= jnp.arange(SEQ_LEN)[None, :]
    scores = jnp.einsum('bqe,bse->bqs', q_head, k_head) * (HEAD_DIM ** -0.5)
    prob_mat = to_grid(jax.nn.softmax(jnp.where(causal[None], scores, MASK_VALUE), axis=-1))
    return to_grid(jnp.einsum('bqs,bse->bqe', prob_mat, v_head))


def attention(queries, key_vals, value_vals):
    head_major = jnp.moveaxis(queries, 2, 0)
    kv_index = jnp.arange(N_HEADS) // GROUP_SIZE
    saved_head = jax.checkpoint(head_attention)

    def one_head(operand):
        q_head, kv_id = operand
        k_head = lax.dynamic_index_in_dim(key_vals, kv_id, axis=2, keepdims=False)
        v_head = lax.dynamic_index_in_dim(value_vals, kv_id, axis=2, keepdims=False)
        return saved_head(q_head, k_head, v_head)

    per_head = lax.map(one_head, (head_major, kv_index))
    return jnp.moveaxis(per_head, 0, 2)


def block_forward(hidden_f, gain, w_qkv_f, w_out_f, cos_t, sin_t):
    inv_rms = lax.rsqrt(jnp.mean(hidden_f * hidden_f, axis=-1, keepdims=True) + NORM_EPS)
    normed = to_grid(hidden_f * inv_rms * gain)
    fused_qkv = jnp.dot(normed.reshape(N_BATCH * SEQ_LEN, D_MODEL), w_qkv_f, preferred_element_type=jnp.float32)
    fused_qkv = fused_qkv.reshape(N_BATCH, SEQ_LEN, QKV_WIDTH)
    queries = fused_qkv[..., :Q_WIDTH].reshape(N_BATCH, SEQ_LEN, N_HEADS, HEAD_DIM)
    key_vals = fused_qkv[..., Q_WIDTH:Q_WIDTH + KV_WIDTH].reshape(N_BATCH, SEQ_LEN, N_KV_HEADS, HEAD_DIM)
    value_vals = fused_qkv[..., Q_WIDTH + KV_WIDTH:].reshape(N_BATCH, SEQ_LEN, N_KV_HEADS, HEAD_DIM)
    attn_out = attention(to_grid(rotate(queries, cos_t, sin_t)), to_grid(rotate(key_vals, cos_t, sin_t)), to_grid(value_vals))
    projected = jnp.dot(attn_out.reshape(N_BATCH * SEQ_LEN, Q_WIDTH), w_out_f.reshape(Q_WIDTH, D_MODEL), preferred_element_type=jnp.float32)
    return (hidden_f + projected.reshape(N_BATCH, SEQ_LEN, D_MODEL)).astype(jnp.bfloat16)


def reference(hidden, norm_w, w_qkv, w_out, long_factor, grad_out):
    cos_t, sin_t = rope_tables(long_factor)

    def forward(hidden_f, gain, w_qkv_f, w_out_f):
        return block_forward(hidden_f, gain, w_qkv_f, w_out_f, cos_t, sin_t)

    block_out, pullback = jax.vjp(forward, hidden.astype(jnp.float32), norm_w.astype(jnp.float32), w_qkv.astype(jnp.float32), w_out.astype(jnp.float32))
    grad_hidden, grad_norm_w, grad_w_qkv, grad_w_out = pullback(grad_out)
    return (block_out, grad_hidden.astype(jnp.bfloat16), grad_w_qkv, grad_w_out, grad_norm_w)
```

```python
import functools
import math
import jax
import jax.numpy as jnp
from jax import lax
from jax.experimental import pallas as pl
from jax.experimental.pallas import tpu as pltpu
from jax.sharding import PartitionSpec as P

NORM_EPS = 1e-5
ROPE_BASE = 10000.0
ROPE_GAIN = math.sqrt(1.0 + math.log(32.0) / math.log(4096.0))
MASK_VALUE = -1e30
BLK = 256
LANES = 128
HEADS = 8
Q_COLS = 4 * LANES
PAIR_W = Q_COLS + 2 * LANES
K_COLS, V_COLS = pl.ds(Q_COLS, LANES), pl.ds(Q_COLS + LANES, LANES)
MESH = pl.DeviceIdType.MESH
VMEM_LIMIT = 67_000_000
COST_BYTES = 2**26
COST_FLOPS = 10**11


def rope_tables(seq_len, long_factor):
    half_rot = long_factor.shape[0]
    exponent = jnp.arange(half_rot, dtype=jnp.float32) / half_rot
    inv_freq = 1.0 / (long_factor * jnp.power(ROPE_BASE, exponent))
    angles = jnp.arange(seq_len, dtype=jnp.float32)[:, None] * inv_freq[None, :]
    cos_t, sin_t = jnp.cos(angles) * ROPE_GAIN, jnp.sin(angles) * ROPE_GAIN
    return (jnp.concatenate([cos_t, cos_t, cos_t, cos_t], axis=1),
            jnp.concatenate([-sin_t, sin_t, -sin_t, sin_t], axis=1))


def lane_rotate(vals, cos_v, sin_v):
    first = lax.broadcasted_iota(jnp.int32, vals.shape, 1) % 64 < 32
    partner = jnp.where(first, pltpu.roll(vals, LANES - 32, 1), pltpu.roll(vals, 32, 1))
    return vals * cos_v + partner * sin_v


def half_variants(vals, out_ref, rows):
    low = lax.broadcasted_iota(jnp.int32, vals.shape, 1) < 64
    swapped = pltpu.roll(vals, 64, 1)
    zero = jnp.zeros_like(vals)
    out_ref[0, rows, :] = jnp.where(low, vals, zero).astype(jnp.bfloat16)
    out_ref[1, rows, :] = jnp.where(low, zero, swapped).astype(jnp.bfloat16)
    out_ref[2, rows, :] = jnp.where(low, swapped, zero).astype(jnp.bfloat16)
    out_ref[3, rows, :] = jnp.where(low, zero, vals).astype(jnp.bfloat16)


def over_keys(reduce, vals):
    return reduce(vals, axis=0, keepdims=True)


def aligned(start, size):
    return pl.ds(pl.multiple_of(start, size), size)


def dot_nt(a, b):
    return lax.dot_general(a, b, (((1,), (1,)), ((), ())), preferred_element_type=jnp.float32)


def dot_nn(a, b):
    return lax.dot_general(a, b, (((1,), (0,)), ((), ())), preferred_element_type=jnp.float32)


def causal_diag(scores):
    keys = lax.broadcasted_iota(jnp.int32, scores.shape, 0)
    rows = lax.broadcasted_iota(jnp.int32, scores.shape, 1)
    return jnp.where(keys <= rows, scores, MASK_VALUE)


def load_weights(w_hbm, w_s, sem):
    width = w_hbm.shape[1]
    n_pairs = width // PAIR_W
    copies = []
    for pair in range(n_pairs):
        for src, dst, cols in ((pair * Q_COLS, 0, Q_COLS), (n_pairs * Q_COLS + pair * LANES, Q_COLS, LANES),
                               (width - (n_pairs - pair) * LANES, Q_COLS + LANES, LANES)):
            copies.append(pltpu.make_async_copy(w_hbm.at[:, pl.ds(src, cols)], w_s.at[:, pl.ds(pair * PAIR_W + dst, cols)], sem.at[len(copies)]))
    return copies


def greet_all(me, n_devs):
    barrier = pltpu.get_barrier_semaphore()
    for k in range(1, n_devs):
        pl.semaphore_signal(barrier, inc=1, device_id={'sp': lax.rem(me + k, n_devs)}, device_id_type=MESH)
    pl.semaphore_wait(barrier, n_devs - 1)


def enter_kernel(hidden, grad_out, gain_ref, w_hbm, x_out, gy_out, qkv_out, turned_out, x_s, own_s, w_s, h_s, turned_s, stage,
                 x_send, x_recv, gy_send, gy_recv, w_sem, out_sem, stage_sem):
    n_devs, tok, d_model = hidden.shape
    me = lax.axis_index('sp')

    def to_peer(src, dst, send_sem, recv_sem, k):
        peer = lax.rem(me + k, n_devs)
        return pltpu.make_async_remote_copy(src_ref=src.at[peer], dst_ref=dst.at[me], send_sem=send_sem.at[k], recv_sem=recv_sem.at[k],
                                            device_id={'sp': peer}, device_id_type=MESH)

    weights = load_weights(w_hbm, w_s, w_sem)
    own_x = pltpu.make_async_copy(hidden.at[me], x_s.at[me], x_send.at[0])
    own_in = pltpu.make_async_copy(grad_out.at[me], own_s, gy_send.at[0])
    own_out = pltpu.make_async_copy(own_s, gy_out.at[me], gy_recv.at[0])
    greet_all(me, n_devs)
    peers = range(1, n_devs)
    xs = [to_peer(hidden, x_s, x_send, x_recv, k) for k in peers]
    gys = [to_peer(grad_out, gy_out, gy_send, gy_recv, k) for k in peers]
    for copy in xs + gys + [own_x, own_in] + weights:
        copy.start()
    gain = gain_ref[...]

    def norm_block(block):
        def norm_rows(n, carry):
            rows = aligned(n * 16, 16)
            x_f = x_s[block, rows, :].astype(jnp.float32)
            inv_rms = lax.rsqrt(jnp.mean(x_f * x_f, axis=-1, keepdims=True) + NORM_EPS)
            h_s[block, rows, :] = (x_f * inv_rms * gain).astype(jnp.bfloat16)
            return carry
        lax.fori_loop(0, tok // 16, norm_rows, 0)

    own_x.wait()
    norm_block(me)
    for k, copy in zip(peers, xs):
        copy.wait()
        norm_block(lax.rem(me + n_devs - k, n_devs))
    own_in.wait()
    own_out.start()
    for copy in weights:
        copy.wait()
    keep_x = pltpu.make_async_copy(x_s, x_out, out_sem.at[0])
    keep_x.start()

    def keep_qkv(pair):
        return pltpu.make_async_copy(stage.at[pair % 2], qkv_out.at[:, pl.ds(pair * PAIR_W, PAIR_W)], stage_sem.at[pair % 2])

    half = n_devs // 2
    n_pairs = w_hbm.shape[1] // PAIR_W
    for pair in range(n_pairs):
        if pair > 1:
            keep_qkv(pair - 2).wait()

        def columns(n, carry):
            for m in range(2):
                left = h_s[pl.ds(m * half, half)].reshape(half * tok, d_model)
                stage[pair % 2, pl.ds(m * half * tok, half * tok), aligned(n * BLK, BLK)] = dot_nn(left, w_s[:, aligned(pair * PAIR_W + n * BLK, BLK)])
            return carry

        lax.fori_loop(0, PAIR_W // BLK, columns, 0)
        keep_qkv(pair).start()

    def turn(n, carry):
        cols = aligned(n * LANES, LANES)
        for block in range(n_devs):
            turned_s[cols, pl.ds(block * tok, tok)] = jnp.transpose(h_s[block, :, cols])
        return carry

    lax.fori_loop(0, d_model // LANES, turn, 0)
    keep_turned = pltpu.make_async_copy(turned_s, turned_out, out_sem.at[1])
    keep_turned.start()
    for copy in gys:
        copy.wait()
    for pair in range(n_pairs - 2, n_pairs):
        keep_qkv(pair).wait()
    keep_turned.wait()
    keep_x.wait()
    own_out.wait()


def enter(hidden, grad_out, gain, w_qkv):
    n_devs, tok, d_model = hidden.shape
    seq, width = n_devs * tok, w_qkv.shape[1]
    anywhere, vmem, dma = pl.BlockSpec(memory_space=pl.ANY), pltpu.VMEM, pltpu.SemaphoreType.DMA
    shape, bf16 = jax.ShapeDtypeStruct, jnp.bfloat16
    return pl.pallas_call(
        enter_kernel,
        in_specs=[anywhere, anywhere, pl.BlockSpec(memory_space=vmem), anywhere],
        out_specs=[anywhere] * 4,
        out_shape=[shape(hidden.shape, bf16), shape(hidden.shape, bf16), shape((seq, width), jnp.float32), shape((d_model, seq), bf16)],
        scratch_shapes=[vmem(hidden.shape, bf16), vmem((tok, d_model), bf16), vmem(w_qkv.shape, bf16), vmem(hidden.shape, bf16),
                        vmem((d_model, seq), bf16), vmem((2, seq, PAIR_W), jnp.float32)]
        + [dma((n_devs,))] * 4 + [dma((3 * width // PAIR_W,)), dma((2,)), dma((2,))],
        compiler_params=pltpu.CompilerParams(vmem_limit_bytes=VMEM_LIMIT, collective_id=2, has_side_effects=True),
        cost_estimate=pl.CostEstimate(flops=COST_FLOPS, bytes_accessed=COST_BYTES, transcendentals=COST_BYTES),
        name="enter",
    )(hidden, grad_out, gain, w_qkv)


def axis_bits():
    me = lax.axis_index('sp')
    coord = {1: lax.rem(me, 2), 2: lax.rem(lax.div(me, 2), 2), 4: lax.div(me, 4)}
    return coord, {bit: {'sp': me + bit * (1 - 2 * coord[bit])} for bit in (1, 2, 4)}


def entry_barrier(peers):
    barrier = pltpu.get_barrier_semaphore()
    for bit in (1, 2, 4):
        pl.semaphore_signal(barrier, inc=1, device_id=peers[bit], device_id_type=MESH)
    pl.semaphore_wait(barrier, 3)


ORDER_OF_HALF = ((2, 4), (4, 2))


def add_rows(dst_ref, a_ref, a_row, b_ref, b_row):
    def body(i, carry):
        step = pl.multiple_of(i * 16, 16)
        total = a_ref[aligned(a_row + step, 16), :] + b_ref[aligned(b_row + step, 16), :].astype(jnp.float32)
        dst_ref[pl.ds(step, 16), :] = total.astype(dst_ref.dtype)
        return carry
    lax.fori_loop(0, dst_ref.shape[0] // 16, body, 0)


class Reduce:
    def __init__(self, coord, peers, sent, own, total, scratch):
        self.coord, self.peers, self.sent, self.own, self.total = coord, peers, sent, own, total
        n = len(sent)
        self.recv_c, self.sum0, self.snd0, self.recv0, self.sum1, self.snd1, self.recv1 = (scratch[k * n:(k + 1) * n] for k in range(7))
        self.send_sem, self.recv_sem = scratch[7 * n:]
        self.n = n

    def copy(self, src, dst, sem, bit):
        return pltpu.make_async_remote_copy(src_ref=src, dst_ref=dst, send_sem=self.send_sem.at[sem], recv_sem=self.recv_sem.at[sem],
                                            device_id=self.peers[bit], device_id_type=MESH)

    def stage_c(self):
        return [self.copy(self.sent[t], self.recv_c[t], t, 1) for t in range(self.n)]

    def stage_s(self, k):
        snd, recv = (self.snd0, self.recv0) if k == 0 else (self.snd1, self.recv1)
        return [self.copy(snd[t].at[h], recv[t].at[h], self.n + 2 * self.n * k + 2 * t + h, ORDER_OF_HALF[h][k])
                for t in range(self.n) for h in range(2)]

    def start(self):
        for copy in self.stage_c():
            copy.start()

    def mid1(self):
        for copy in self.stage_c():
            copy.wait()
        for t in range(self.n):
            half = self.own[t].shape[0] // 2
            for h in range(2):
                c = self.coord[ORDER_OF_HALF[h][0]]
                row = h * half + (1 - c) * (half // 2)
                add_rows(self.snd0[t].at[h], self.own[t], row, self.recv_c[t], row)
        for copy in self.stage_s(0):
            copy.start()
        for t in range(self.n):
            half = self.own[t].shape[0] // 2
            for h in range(2):
                row = h * half + self.coord[ORDER_OF_HALF[h][0]] * (half // 2)
                add_rows(self.sum0[t].at[h], self.own[t], row, self.recv_c[t], row)

    def mid2(self):
        for copy in self.stage_s(0):
            copy.wait()
        for t in range(self.n):
            quarter = self.own[t].shape[0] // 4
            for h in range(2):
                row = (1 - self.coord[ORDER_OF_HALF[h][1]]) * (quarter // 2)
                add_rows(self.snd1[t].at[h], self.sum0[t].at[h], row, self.recv0[t].at[h], row)
        for copy in self.stage_s(1):
            copy.start()
        for t in range(self.n):
            quarter = self.own[t].shape[0] // 4
            for h in range(2):
                row = self.coord[ORDER_OF_HALF[h][1]] * (quarter // 2)
                add_rows(self.sum1[t].at[h], self.sum0[t].at[h], row, self.recv0[t].at[h], row)

    def end(self):
        for copy in self.stage_s(1):
            copy.wait()
        for t in range(self.n):
            for h in range(2):
                add_rows(self.total[t].at[h], self.sum1[t].at[h], 0, self.recv1[t].at[h], 0)

    @staticmethod
    def scratch_shapes(shapes):
        vmem = lambda dtype, div: [pltpu.VMEM((2, r // div, c) if div else (r, c), dtype) for r, c in shapes]
        n = len(shapes)
        return (vmem(jnp.bfloat16, 0) + vmem(jnp.float32, 4) + vmem(jnp.bfloat16, 4) + vmem(jnp.bfloat16, 4)
                + vmem(jnp.float32, 8) + vmem(jnp.bfloat16, 8) + vmem(jnp.bfloat16, 8)
                + [pltpu.SemaphoreType.DMA((5 * n,)), pltpu.SemaphoreType.DMA((5 * n,))])


class Gather:
    def __init__(self, peers, total, pieces, scratch):
        self.peers, self.total, self.pieces = peers, total, pieces
        self.send_sem, self.recv_sem, self.local_sem = scratch
        self.n = len(total)

    def copy(self, src, dst, sem, bit):
        return pltpu.make_async_remote_copy(src_ref=src, dst_ref=dst, send_sem=self.send_sem.at[sem], recv_sem=self.recv_sem.at[sem],
                                            device_id=self.peers[bit], device_id_type=MESH)

    def stage(self, k):
        copies = []
        for t in range(self.n):
            if k == 2:
                copies.append(self.copy(self.pieces[t].at[pl.ds(0, 8)], self.pieces[t].at[pl.ds(8, 8)], 4 * self.n + t, 1))
                continue
            for h in range(2):
                if k == 0:
                    src, dst = self.total[t].at[pl.ds(h, 1)], self.pieces[t].at[pl.ds(4 * h + 1, 1)]
                else:
                    src, dst = self.pieces[t].at[pl.ds(4 * h, 2)], self.pieces[t].at[pl.ds(4 * h + 2, 2)]
                copies.append(self.copy(src, dst, 2 * self.n * k + 2 * t + h, ORDER_OF_HALF[h][1 - k]))
        return copies

    def local(self):
        return [pltpu.make_async_copy(self.total[t].at[pl.ds(h, 1)], self.pieces[t].at[pl.ds(4 * h, 1)], self.local_sem.at[2 * t + h])
                for t in range(self.n) for h in range(2)]

    def start(self):
        for copy in self.stage(0) + self.local():
            copy.start()

    def mid1(self):
        for copy in self.stage(0) + self.local():
            copy.wait()
        for copy in self.stage(1):
            copy.start()

    def mid2(self):
        for copy in self.stage(1):
            copy.wait()
        for copy in self.stage(2):
            copy.start()

    def end(self):
        for copy in self.stage(2):
            copy.wait()

    @staticmethod
    def scratch_shapes(n):
        return [pltpu.SemaphoreType.DMA((5 * n,)), pltpu.SemaphoreType.DMA((5 * n,)), pltpu.SemaphoreType.DMA((2 * n,))]


def attn_kernel(qkv_ref, wo_ref, cos_ref, sin_ref, normed_ref, gy_ref,
                o_ref, out_ref, sent_q_out, sent_d_out, own_q_out, own_d_out, total_q_out, total_d_out, pieces_q, pieces_d, *scratch):
    scratch = list(scratch)
    take = lambda n: [scratch.pop(0) for _ in range(n)]
    q_s, do_s, k_var, v_var, k_t, v_t, ot_ref, dq_t, dk_acc, dv_acc = take(10)
    sent, own, total = take(2), take(2), take(2)
    pair = pl.program_id(0)
    coord, peers = axis_bits()
    reduce = Reduce(coord, peers, sent, own, total, take(16))
    gather = Gather(peers, total, [ref.at[jnp.maximum(pair - 2, 0)] for ref in (pieces_q, pieces_d)], take(3))
    turn_sem, out_sem = take(2)

    @pl.when(pair == 0)
    def _():
        entry_barrier(peers)

    @pl.when(pair > 0)
    def _():
        for n, bit in enumerate((1, 2, 4)):
            pl.semaphore_signal(turn_sem.at[n], inc=1, device_id=peers[bit], device_id_type=MESH)
        for n in range(3):
            pl.semaphore_wait(turn_sem.at[n], 1)
        reduce.start()

    @pl.when(pair > 1)
    def _():
        gather.start()

    def middle(first):
        @pl.when(pair > 0)
        def _():
            (reduce.mid1 if first else reduce.mid2)()

        @pl.when(pair > 1)
        def _():
            (gather.mid1 if first else gather.mid2)()

    seq = qkv_ref.shape[0]
    n_blk = seq // BLK

    def setup_block(i, carry):
        rows = aligned(i * LANES, LANES)
        cos_v, sin_v = cos_ref[rows, :], sin_ref[rows, :]
        for c in range(4):
            cols = pl.ds(c * LANES, LANES)
            q_s[c, rows, :] = (lane_rotate(qkv_ref[rows, cols], cos_v, sin_v) * 0.125).astype(jnp.bfloat16)
        k_rot = lane_rotate(qkv_ref[rows, K_COLS], cos_v, sin_v).astype(jnp.bfloat16).astype(jnp.float32)
        half_variants(k_rot, k_var, rows)
        k_t[:, rows] = jnp.transpose(k_rot).astype(jnp.bfloat16)
        v_val = qkv_ref[rows, V_COLS].astype(jnp.bfloat16).astype(jnp.float32)
        half_variants(v_val, v_var, rows)
        v_t[:, rows] = jnp.transpose(v_val).astype(jnp.bfloat16)
        return carry

    lax.fori_loop(0, seq // LANES, setup_block, 0)

    def grad_attn(n, carry):
        heads = aligned(n * 256, 256)
        for m in range(seq // 512):
            rows = pl.ds(m * 512, 512)
            block = dot_nt(gy_ref[rows, :], wo_ref[heads, :]).astype(jnp.bfloat16)
            do_s[2 * n, rows, :] = block[:, :LANES]
            do_s[2 * n + 1, rows, :] = block[:, LANES:]
        return carry

    lax.fori_loop(0, 2, grad_attn, 0)
    middle(True)
    dk_acc[...] = jnp.zeros_like(dk_acc)
    dv_acc[...] = jnp.zeros_like(dv_acc)
    half = lax.broadcasted_iota(jnp.int32, (BLK, LANES), 1) // 64

    def head_pair(hp, carry):
        kv = hp // 2
        sub_kv = pl.multiple_of(kv * 64, 64)
        for i in range(n_blk):
            rows = pl.ds(i * BLK, BLK)
            q_blk = q_s[hp, rows, :]
            do_blk = do_s[hp, rows, :]
            parts = [(pl.ds(i * BLK, BLK), True)]
            if i:
                parts.append((pl.ds(0, i * BLK), False))
            dv_sum, dk_sum = [0.0] * len(parts), [0.0] * len(parts)
            for par in range(2):
                var = kv * 2 + par
                sub_h = aligned(hp * LANES + par * 64, 64)
                q_mine = jnp.where(half == par, q_blk, jnp.zeros_like(q_blk))
                do_mine = jnp.where(half == par, do_blk, jnp.zeros_like(do_blk))
                scores, top = [], None
                for keys, is_diag in parts:
                    part = dot_nt(k_var[var, keys, :], q_blk)
                    if is_diag:
                        part = causal_diag(part)
                    scores.append(part)
                    part_top = over_keys(jnp.max, part)
                    top = part_top if top is None else jnp.maximum(top, part_top)
                exps = [jnp.exp(part - top) for part in scores]
                inv = 1.0 / sum(over_keys(jnp.sum, part) for part in exps)
                probs, grads, row_dot, attn = [], [], 0.0, 0.0
                for n, (keys, _) in enumerate(parts):
                    prob = exps[n] * inv
                    prob_b = prob.astype(jnp.bfloat16)
                    grad_p = dot_nt(v_var[var, keys, :], do_blk)
                    row_dot = row_dot + over_keys(jnp.sum, prob * grad_p)
                    attn = attn + dot_nn(v_t[pl.ds(sub_kv, 64), keys], prob_b)
                    dv_sum[n] = dv_sum[n] + dot_nn(prob_b, do_mine)
                    probs.append(prob)
                    grads.append(grad_p)
                ot_ref[sub_h, rows] = attn.astype(jnp.bfloat16)
                acc = 0.0
                for n, (keys, _) in enumerate(parts):
                    grad_s = (probs[n] * (grads[n] - row_dot)).astype(jnp.bfloat16)
                    dk_sum[n] = dk_sum[n] + dot_nn(grad_s, q_mine)
                    acc = acc + dot_nn(k_t[pl.ds(sub_kv, 64), keys], grad_s)
                dq_t[sub_h, rows] = acc
            for n, (keys, _) in enumerate(parts):
                dv_acc[kv, keys, :] += dv_sum[n]
                dk_acc[kv, keys, :] += dk_sum[n]
        return carry

    lax.fori_loop(0, HEADS // 2, head_pair, 0)

    def finish_block(i, carry):
        rows = aligned(i * LANES, LANES)
        cos_v, sin_v = cos_ref[rows, :], -sin_ref[rows, :]
        for c in range(4):
            cols = pl.ds(c * LANES, LANES)
            o_ref[rows, cols] = jnp.transpose(ot_ref[cols, rows])
            grad_q = jnp.transpose(dq_t[cols, rows]) * 0.125
            out_ref[rows, cols] = lane_rotate(grad_q, cos_v, sin_v).astype(jnp.bfloat16)
        low = lax.broadcasted_iota(jnp.int32, (LANES, LANES), 1) < 64
        merged = []
        for acc_ref in (dk_acc, dv_acc):
            first, second = acc_ref[0, rows, :], acc_ref[1, rows, :]
            merged.append(jnp.where(low, first + pltpu.roll(first, 64, 1), second + pltpu.roll(second, 64, 1)))
        out_ref[rows, K_COLS] = lane_rotate(merged[0], cos_v, sin_v).astype(jnp.bfloat16)
        out_ref[rows, V_COLS] = merged[1].astype(jnp.bfloat16)
        return carry

    lax.fori_loop(0, seq // LANES, finish_block, 0)
    mine = coord[1]
    rows_q, rows_d = own[0].shape[0], own[1].shape[0]

    def weight_q(n, carry):
        cols = aligned(n * 256, 256)
        for m in range(rows_q // 512):
            rows = pl.ds(m * 512, 512)
            for half, ref in ((1 - mine, sent[0]), (mine, own[0])):
                left = normed_ref[aligned(half * rows_q + m * 512, 512), :]
                ref[rows, cols] = dot_nn(left, out_ref[:, cols]).astype(ref.dtype)
        return carry

    def weight_d(n, carry):
        cols = aligned(n * 256, 256)
        for half, ref in ((1 - mine, sent[1]), (mine, own[1])):
            left = ot_ref[aligned(half * rows_d, rows_d), :]
            ref[:, cols] = dot_nn(left, gy_ref[:, cols]).astype(ref.dtype)
        return carry

    middle(False)
    lax.fori_loop(0, PAIR_W // 256, weight_q, 0)
    lax.fori_loop(0, gy_ref.shape[1] // 256, weight_d, 0)

    @pl.when(pair > 0)
    def _():
        reduce.end()

    @pl.when(pair > 1)
    def _():
        gather.end()

    @pl.when(pair == pl.num_programs(0) - 1)
    def _():
        outs = [sent_q_out, sent_d_out, own_q_out, own_d_out, total_q_out, total_d_out]
        copies = [pltpu.make_async_copy(src, dst, out_sem.at[n]) for n, (src, dst) in enumerate(zip(sent + own + total, outs))]
        for copy in copies:
            copy.start()
        for copy in copies:
            copy.wait()


def total_shapes(own):
    return [jax.ShapeDtypeStruct((2, o.shape[0] // 8, o.shape[1]), jnp.bfloat16) for o in own]


def piece_shapes(total):
    return [jax.ShapeDtypeStruct((16,) + t.shape[1:], jnp.bfloat16) for t in total]


def attention(qkv, w_o, cos_t, sin_t, normed_t, grad_y):
    seq, d_model = grad_y.shape
    n_pairs = qkv.shape[1] // PAIR_W
    q_cols = HEADS * 64
    const = lambda shape: pl.BlockSpec(shape, lambda p: (0,) * len(shape), pipeline_mode=pl.Buffered(1))
    col = lambda width: pl.BlockSpec((seq, width), lambda p: (0, p))
    anywhere = pl.BlockSpec(memory_space=pl.ANY)
    shape = jax.ShapeDtypeStruct
    slab = pltpu.VMEM((4, seq, LANES), jnp.bfloat16)
    turned = pltpu.VMEM((LANES, seq), jnp.bfloat16)
    acc = pltpu.VMEM((2, seq, LANES), jnp.float32)
    partial = [(d_model // 2, PAIR_W), (q_cols // 2, d_model)]
    own = [shape(p, jnp.float32) for p in partial]
    sent = [shape(p, jnp.bfloat16) for p in partial]
    totals = total_shapes(own)
    pieces = [shape((n_pairs - 2,) + p.shape, p.dtype) for p in piece_shapes(totals)]
    kept = [pltpu.VMEM(p.shape, p.dtype) for p in sent + own + totals]
    out = pl.pallas_call(
        attn_kernel,
        grid=(n_pairs,),
        in_specs=[col(PAIR_W), pl.BlockSpec((q_cols, d_model), lambda p: (p, 0)), const((seq, LANES)), const((seq, LANES)), const((d_model, seq)), const((seq, d_model))],
        out_specs=[col(q_cols), col(PAIR_W)] + [anywhere] * 8,
        out_shape=[shape((seq, q_cols * n_pairs), jnp.bfloat16), shape((seq, PAIR_W * n_pairs), jnp.bfloat16)] + sent + own + totals + pieces,
        scratch_shapes=[slab, slab, slab, slab, turned, turned, pltpu.VMEM((q_cols, seq), jnp.bfloat16), pltpu.VMEM((q_cols, seq), jnp.float32), acc, acc]
        + kept + Reduce.scratch_shapes(partial) + Gather.scratch_shapes(2)
        + [pltpu.SemaphoreType.REGULAR((3,)), pltpu.SemaphoreType.DMA((6,))],
        compiler_params=pltpu.CompilerParams(vmem_limit_bytes=VMEM_LIMIT, collective_id=0, has_side_effects=True),
        cost_estimate=pl.CostEstimate(flops=COST_FLOPS, bytes_accessed=COST_BYTES, transcendentals=COST_BYTES),
        name="attn",
    )(qkv, w_o, cos_t, sin_t, normed_t, grad_y)
    return out[0], out[1], (list(out[2:4]), list(out[4:6])), list(out[6:8]), out[8:10]


def finish_kernel(o_ref, x_ref, grads_ref, gy_ref, gain_ref, wo_ref, w_hbm, sent_q, sent_d, own_q, own_d, old_q, old_d,
                  y_out, gh_out, old_pieces_q, old_pieces_d, pieces_q, pieces_d, norm_out, *scratch):
    scratch = list(scratch)
    take = lambda n: [scratch.pop(0) for _ in range(n)]
    y_s, gh_s, w_s, dh_s, norm_ref, norm_row, norm_all = take(7)
    total = take(2)
    step = pl.program_id(0)
    me = lax.axis_index('sp')
    coord, peers = axis_bits()
    reduce = Reduce(coord, peers, [sent_q, sent_d], [own_q, own_d], total, take(16))
    gather = Gather(peers, [old_q, old_d], [old_pieces_q, old_pieces_d], take(3))
    last = Gather(peers, total, [pieces_q, pieces_d], take(3))
    w_sem, y_send, y_recv, gh_send, gh_recv, norm_send, norm_recv = take(7)
    n_devs = y_out.shape[0]
    tok = y_out.shape[1]
    half_steps = pl.num_programs(0) // 2
    per_step = n_devs // half_steps
    weights = load_weights(w_hbm, w_s, w_sem)

    def share(values, out, send_sem, recv_sem, dest, act):
        @pl.when(dest == me)
        def _():
            act(pltpu.make_async_copy(values.at[dest], out.at[dest], send_sem.at[dest]), True)

        @pl.when(dest != me)
        def _():
            act(pltpu.make_async_remote_copy(src_ref=values.at[dest], dst_ref=out.at[me], send_sem=send_sem.at[dest], recv_sem=recv_sem.at[me],
                                             device_id={'sp': dest}, device_id_type=MESH), False)

    def send(values, out, send_sem, recv_sem, dests):
        for dest in dests:
            share(values, out, send_sem, recv_sem, dest, lambda copy, local: copy.start())

    def finish(values, out, send_sem, recv_sem):
        for peer in range(n_devs):
            @pl.when(peer == me)
            def _():
                pltpu.make_async_copy(values.at[peer], out.at[peer], send_sem.at[peer]).wait()

            @pl.when(peer != me)
            def _():
                pltpu.make_async_remote_copy(src_ref=values.at[peer], dst_ref=out.at[peer], send_sem=send_sem.at[peer], recv_sem=recv_sem.at[peer],
                                             device_id={'sp': peer}, device_id_type=MESH).wait()

    def share_norm(act):
        for k in range(1, n_devs):
            peer = lax.rem(me + k, n_devs)
            copy = pltpu.make_async_remote_copy(src_ref=norm_row, dst_ref=norm_all.at[me], send_sem=norm_send.at[k], recv_sem=norm_recv.at[k],
                                                device_id={'sp': peer}, device_id_type=MESH)
            act(copy)

    @pl.when(step == 0)
    def _():
        greet_all(me, n_devs)
        reduce.start()
        gather.start()
        for copy in weights:
            copy.start()
        norm_ref[...] = jnp.zeros_like(norm_ref)

    @pl.when(step == 1)
    def _():
        reduce.mid1()
        gather.mid1()

    @pl.when(jnp.logical_and(step >= 1, step <= half_steps))
    def _():
        send(y_s, y_out, y_send, y_recv, [(step - 1) * per_step + k for k in range(per_step)])

    d_model = wo_ref.shape[1]

    @pl.when(step < half_steps)
    def _():
        def cols_of_y(n, carry):
            cols = aligned(n * 512, 512)
            block = (x_ref[:, cols].astype(jnp.float32) + dot_nn(o_ref[...], wo_ref[:, cols])).astype(jnp.bfloat16)
            for k in range(per_step):
                y_s[step * per_step + k, :, cols] = block[k * tok:(k + 1) * tok, :]
            return carry
        lax.fori_loop(0, d_model // 512, cols_of_y, 0)

    @pl.when(step == half_steps)
    def _():
        for copy in weights:
            copy.wait()

    @pl.when(step >= half_steps)
    def _():
        def cols_of_dh(n, carry):
            rows = aligned(n * 512, 512)
            dh_s[:, rows] = dot_nt(grads_ref[...], w_s[rows, :])
            return carry
        lax.fori_loop(0, d_model // 512, cols_of_dh, 0)
        gain = gain_ref[...]

        def norm_rows(n, carry):
            rows = aligned(n * 16, 16)
            x_f = x_ref[rows, :].astype(jnp.float32)
            inv_rms = lax.rsqrt(jnp.mean(x_f * x_f, axis=-1, keepdims=True) + NORM_EPS)
            unit = x_f * inv_rms
            grad_normed = dh_s[rows, :]
            grad_unit = grad_normed * gain
            mean_dot = jnp.mean(grad_unit * unit, axis=-1, keepdims=True)
            grad_x = gy_ref[rows, :].astype(jnp.float32) + inv_rms * (grad_unit - unit * mean_dot)
            place = (step - half_steps) * per_step + n // (tok // 16)
            gh_s[place, aligned(lax.rem(n, tok // 16) * 16, 16), :] = grad_x.astype(jnp.bfloat16)
            weighted = grad_normed * unit
            norm_ref[...] += weighted[:8, :] + weighted[8:, :]
            return carry
        lax.fori_loop(0, per_step * tok // 16, norm_rows, 0)

    @pl.when(step == pl.num_programs(0) - 1)
    def _():
        gh = (gh_s, gh_out, gh_send, gh_recv)
        norm_row[...] = over_keys(jnp.sum, norm_ref[...])
        reduce.mid2()
        gather.mid2()
        share_norm(lambda copy: copy.start())
        send(*gh, range(n_devs // 2))
        reduce.end()
        last.start()
        send(*gh, range(n_devs // 2, n_devs))
        gather.end()
        last.mid1()
        last.mid2()
        share_norm(lambda copy: copy.wait())
        norm_all[me] = norm_row[...]
        norm_out[...] = sum(norm_all[peer] for peer in range(n_devs))
        finish(y_s, y_out, y_send, y_recv)
        last.end()
        finish(*gh)


def finish(attn, x, grads, grad_y, gain, w_o, w_qkv, reduce, old_total, n_devs):
    seq, d_model = x.shape
    sent, own = reduce
    steps = 8
    rows = 2 * seq // steps
    tok = seq // n_devs
    const = lambda shape: pl.BlockSpec(shape, lambda s: (0,) * len(shape), pipeline_mode=pl.Buffered(1))
    early = lambda width: pl.BlockSpec((rows, width), lambda s: (jnp.minimum(s, steps // 2 - 1), 0))
    late = lambda width: pl.BlockSpec((rows, width), lambda s: (jnp.maximum(s - steps // 2, 0), 0))
    anywhere = pl.BlockSpec(memory_space=pl.ANY)
    shape = jax.ShapeDtypeStruct
    totals = total_shapes(own)
    tokens = shape((n_devs, tok, d_model), jnp.bfloat16)
    dma = lambda: pltpu.SemaphoreType.DMA((n_devs,))
    out = pl.pallas_call(
        finish_kernel,
        grid=(steps,),
        in_specs=[early(q_w) for q_w in (attn.shape[1],)] + [pl.BlockSpec((rows, d_model), lambda s: (lax.rem(s, steps // 2), 0)), late(grads.shape[1]), late(d_model),
                  const((1, d_model)), const(w_o.shape), anywhere, anywhere, anywhere]
        + [const(o.shape) for o in own] + [const(t.shape) for t in totals],
        out_specs=[anywhere] * 6 + [pl.BlockSpec((1, d_model), lambda s: (0, 0))],
        out_shape=[tokens, tokens] + piece_shapes(totals) + piece_shapes(totals) + [shape((1, d_model), jnp.float32)],
        scratch_shapes=[pltpu.VMEM(tokens.shape, jnp.bfloat16), pltpu.VMEM(tokens.shape, jnp.bfloat16),
                        pltpu.VMEM(w_qkv.shape, jnp.bfloat16), pltpu.VMEM((rows, d_model), jnp.float32),
                        pltpu.VMEM((8, d_model), jnp.float32), pltpu.VMEM((1, d_model), jnp.float32),
                        pltpu.VMEM((n_devs, 1, d_model), jnp.float32)]
        + [pltpu.VMEM(t.shape, t.dtype) for t in totals]
        + Reduce.scratch_shapes([o.shape for o in own]) + Gather.scratch_shapes(2) + Gather.scratch_shapes(2)
        + [pltpu.SemaphoreType.DMA((3 * w_qkv.shape[1] // PAIR_W,))] + [dma()] * 6,
        compiler_params=pltpu.CompilerParams(vmem_limit_bytes=VMEM_LIMIT, collective_id=1, has_side_effects=True),
        cost_estimate=pl.CostEstimate(flops=COST_FLOPS, bytes_accessed=COST_BYTES, transcendentals=COST_BYTES),
        name="finish",
    )(attn, x, grads, grad_y, gain, w_o, w_qkv, *sent, *own, *old_total)
    return out[0], out[1], out[2:4], out[4:6], out[6]


def place_kernel(n_pairs, slots, *refs):
    pieces_q, pieces_d, tokens = refs[:n_pairs], refs[n_pairs:2 * n_pairs], refs[2 * n_pairs:2 * n_pairs + 2]
    q_out, d_out, *tokens_out = refs[2 * n_pairs + 2:]
    for src, dst in zip(tokens, tokens_out):
        dst[...] = src[...]
    for pair in range(n_pairs):
        d_out[pair] = pieces_d[pair][0, 0].astype(jnp.float32)
        for src, dst, width in ((0, pair * 512, 512), (512, n_pairs * 512 + pair * LANES, LANES),
                                (640, n_pairs * 640 + pair * LANES, LANES)):
            q_out[:, dst:dst + width] = pieces_q[pair][0, 0, :, src:src + width].astype(jnp.float32)


def place(slots, parts_q, parts_d, tokens):
    specs, args, sizes = [], [], []
    for parts in (parts_q, parts_d):
        chunks = [(part, c) for part in parts for c in range(part.shape[0])]
        rows, width = parts[0].shape[2:]
        specs += [pl.BlockSpec((1, 1, rows, width), lambda s, slots, c=c: (c, s, 0, 0)) for _, c in chunks]
        args += [part for part, _ in chunks]
        sizes.append((len(chunks), rows, width))
    (n_pairs, rows_q, width_q), (_, rows_d, width_d) = sizes
    flat = [t.reshape(16, -1, t.shape[-1]) for t in tokens]
    through = pl.BlockSpec((1,) + flat[0].shape[1:], lambda s, slots: (s, 0, 0))
    shape = jax.ShapeDtypeStruct
    grad_q, grad_d, *out = pl.pallas_call(
        functools.partial(place_kernel, n_pairs),
        grid_spec=pltpu.PrefetchScalarGridSpec(
            num_scalar_prefetch=1, grid=(16,), in_specs=specs + [through] * 2,
            out_specs=[pl.BlockSpec((rows_q, n_pairs * width_q), lambda s, slots: (slots[s], 0)),
                       pl.BlockSpec((n_pairs, rows_d, width_d), lambda s, slots: (0, slots[s], 0)), through, through]),
        out_shape=[shape((16 * rows_q, n_pairs * width_q), jnp.float32), shape((n_pairs, 16 * rows_d, width_d), jnp.float32)]
        + [shape(t.shape, t.dtype) for t in flat],
        compiler_params=pltpu.CompilerParams(vmem_limit_bytes=VMEM_LIMIT),
        cost_estimate=pl.CostEstimate(flops=COST_FLOPS, bytes_accessed=COST_BYTES, transcendentals=COST_BYTES),
        name="place",
    )(slots, *args, *flat)
    return grad_q, grad_d, [o.reshape(t.shape) for o, t in zip(out, tokens)]


def row_slots():
    me = lax.axis_index('sp')
    core, x, y = me & 1, (me >> 1) & 1, me >> 2
    order = []
    for c in (core, 1 - core):
        for half, (a, b) in enumerate(((x, y), (y, x))):
            for a_i in (a, 1 - a):
                for b_i in (b, 1 - b):
                    order.append(c * 8 + half * 4 + a_i * 2 + b_i)
    return jnp.stack(order).astype(jnp.int32)


def solution(mesh):
    n_devs = mesh.shape['sp']

    def device_step(hidden, norm_w, w_qkv, w_out, long_factor, grad_out):
        d_model = hidden.shape[-1]
        gain = norm_w.astype(jnp.float32)[None]
        x, grad_y, qkv, normed_t = enter(hidden, grad_out, gain, w_qkv)
        x, grad_y = x.reshape(-1, d_model), grad_y.reshape(-1, d_model)
        cos_t, sin_t = rope_tables(len(x), long_factor)
        w_o = w_out.reshape(-1, d_model)
        attn, grads, partial, total, pieces = attention(qkv, w_o, cos_t, sin_t, normed_t, grad_y)
        block_out, grad_hidden, before_last, last, grad_norm_w = finish(attn, x, grads, grad_y, gain, w_o, w_qkv, partial, total, n_devs)
        parts = [[first, second[None], third[None]] for first, second, third in zip(pieces, before_last, last)]
        grad_w_qkv, grad_w_out, (block_out, grad_hidden) = place(row_slots(), *parts, (block_out, grad_hidden))
        return block_out, grad_hidden, grad_w_qkv, grad_w_out.reshape(w_out.shape), grad_norm_w.reshape(-1)

    tok_spec = P('dp', 'sp', None)
    return jax.shard_map(device_step, mesh=mesh,
                         in_specs=(tok_spec, P(), P(), P(), P(), tok_spec),
                         out_specs=(tok_spec, tok_spec, P('dp', None), P('dp', None, None), P('dp')),
                         check_vma=False)
```

```python
import functools
import math
import jax
import jax.numpy as jnp
from jax import lax
from jax.experimental import pallas as pl
from jax.experimental.pallas import tpu as pltpu
from jax.sharding import PartitionSpec as P

NORM_EPS = 1e-5
ROPE_BASE = 10000.0
ROPE_GAIN = math.sqrt(1.0 + math.log(32.0) / math.log(4096.0))
MASK_VALUE = -1e30
BLK = 256
TALL = 512
LANES = 128
HEAD = LANES // 2
Q_COLS = 2 * LANES
GROUP_W = Q_COLS + LANES
PAIR_W = 2 * GROUP_W
KV_COLS = pl.ds(Q_COLS, LANES)
MESH = pl.DeviceIdType.MESH
VMEM_LIMIT = 67_000_000
COST_BYTES = 2**26
COST_FLOPS = 10**11


def inverse_frequencies(long_factor):
    half_rot = long_factor.shape[0]
    exponent = jnp.arange(half_rot, dtype=jnp.float32) / half_rot
    inv_freq = 1.0 / (long_factor * jnp.power(ROPE_BASE, exponent))
    return jnp.tile(inv_freq, LANES // half_rot)[None]


def first_quarter(shape):
    return lax.broadcasted_iota(jnp.int32, shape, 1) % HEAD < HEAD // 2


def lane_rotate(vals, cos_v, sin_v):
    first = first_quarter(vals.shape)
    partner = jnp.where(first, pltpu.roll(vals, LANES - 32, 1), pltpu.roll(vals, 32, 1))
    return vals * cos_v + partner * sin_v


def low_half(shape):
    return lax.broadcasted_iota(jnp.int32, shape, 1) < HEAD


def cross(a, b):
    low = low_half(a.shape)
    return jnp.where(low, a, pltpu.roll(b, HEAD, 1)), jnp.where(low, pltpu.roll(a, HEAD, 1), b)


def half_variants(vals, half, out_ref, turned_ref, rows):
    low = low_half(vals.shape)
    swapped = pltpu.roll(vals, HEAD, 1)
    first, second = jnp.where(half == 0, vals, swapped), jnp.where(half == 0, swapped, vals)
    out_ref[0, rows, :] = jnp.where(low, first, 0.0).astype(jnp.bfloat16)
    out_ref[1, rows, :] = jnp.where(low, 0.0, second).astype(jnp.bfloat16)
    turned_ref[:, rows] = jnp.transpose(first)[:HEAD].astype(jnp.bfloat16)


def over_keys(reduce, vals):
    return reduce(vals, axis=0, keepdims=True)


def aligned(start, size):
    return pl.ds(pl.multiple_of(start, size), size)


def dot_nt(a, b):
    return lax.dot_general(a, b, (((1,), (1,)), ((), ())), preferred_element_type=jnp.float32)


def dot_nn(a, b):
    return lax.dot_general(a, b, (((1,), (0,)), ((), ())), preferred_element_type=jnp.float32)


def causal_diag(scores):
    keys = lax.broadcasted_iota(jnp.int32, scores.shape, 0)
    rows = lax.broadcasted_iota(jnp.int32, scores.shape, 1)
    return jnp.where(keys <= rows, scores, MASK_VALUE)


def load_weights(w_hbm, w_s, sem, places):
    width = w_hbm.shape[1]
    n_pairs = width // PAIR_W
    copies = []
    for pair in range(n_pairs):
        q, k, v = pair * 2 * Q_COLS, n_pairs * 2 * Q_COLS + pair * LANES, width - (n_pairs - pair) * LANES
        for src, cols, dst in zip((q, q + Q_COLS, k, v), (Q_COLS, Q_COLS, LANES, LANES), places):
            copies.append(pltpu.make_async_copy(w_hbm.at[:, pl.ds(src, cols)], w_s.at[:, pl.ds(pair * PAIR_W + dst, cols)], sem.at[len(copies)]))
    return copies


def greet_all(me, n_devs):
    barrier = pltpu.get_barrier_semaphore()
    for k in range(1, n_devs):
        pl.semaphore_signal(barrier, inc=1, device_id={'sp': lax.rem(me + k, n_devs)}, device_id_type=MESH)
    pl.semaphore_wait(barrier, n_devs - 1)


def enter_kernel(hidden, grad_out, gain_ref, freq_ref, w_hbm, x_out, gy_out, qkv_out, turned_out, cos_out, sin_out, x_s, own_s, w_s, h_s, turned_s, stage,
                 x_send, x_recv, gy_send, gy_recv, w_sem, out_sem, stage_sem):
    n_devs, tok, d_model = hidden.shape
    me = lax.axis_index('sp')

    def to_peer(src, dst, send_sem, recv_sem, k):
        peer = lax.rem(me + k, n_devs)
        return pltpu.make_async_remote_copy(src_ref=src.at[peer], dst_ref=dst.at[me], send_sem=send_sem.at[k], recv_sem=recv_sem.at[k],
                                            device_id={'sp': peer}, device_id_type=MESH)

    weights = load_weights(w_hbm, w_s, w_sem, (0, Q_COLS, 2 * Q_COLS, PAIR_W - LANES))
    own_x = pltpu.make_async_copy(hidden.at[me], x_s.at[me], x_send.at[0])
    own_in = pltpu.make_async_copy(grad_out.at[me], own_s, gy_send.at[0])
    own_out = pltpu.make_async_copy(own_s, gy_out.at[me], gy_recv.at[0])
    greet_all(me, n_devs)
    peers = range(1, n_devs)
    xs = [to_peer(hidden, x_s, x_send, x_recv, k) for k in peers]
    gys = [to_peer(grad_out, gy_out, gy_send, gy_recv, k) for k in peers]
    for copy in xs + gys + [own_x, own_in] + weights:
        copy.start()
    gain = gain_ref[...]

    def norm_block(block):
        def norm_rows(n, carry):
            rows = aligned(n * 16, 16)
            x_f = x_s[block, rows, :].astype(jnp.float32)
            inv_rms = lax.rsqrt(jnp.mean(x_f * x_f, axis=-1, keepdims=True) + NORM_EPS)
            h_s[block, rows, :] = (x_f * inv_rms * gain).astype(jnp.bfloat16)
            return carry
        lax.fori_loop(0, tok // 16, norm_rows, 0)

    own_x.wait()
    norm_block(me)
    for k, copy in zip(peers, xs):
        copy.wait()
        norm_block(lax.rem(me + n_devs - k, n_devs))
    own_in.wait()
    own_out.start()
    for copy in weights:
        copy.wait()
    keep_x = pltpu.make_async_copy(x_s, x_out, out_sem.at[0])
    keep_x.start()

    def keep_qkv(pair):
        return pltpu.make_async_copy(stage.at[pair % 2], qkv_out.at[:, pl.ds(pair * PAIR_W, PAIR_W)], stage_sem.at[pair % 2])

    half = n_devs // 2
    n_pairs = w_hbm.shape[1] // PAIR_W
    for pair in range(n_pairs):
        if pair > 1:
            keep_qkv(pair - 2).wait()

        def columns(n, carry):
            for m in range(2):
                left = h_s[pl.ds(m * half, half)].reshape(half * tok, d_model)
                stage[pair % 2, pl.ds(m * half * tok, half * tok), aligned(n * BLK, BLK)] = dot_nn(left, w_s[:, aligned(pair * PAIR_W + n * BLK, BLK)])
            return carry

        lax.fori_loop(0, PAIR_W // BLK, columns, 0)
        keep_qkv(pair).start()

    def turn(n, carry):
        cols = aligned(n * LANES, LANES)
        for block in range(n_devs):
            turned_s[cols, pl.ds(block * tok, tok)] = jnp.transpose(h_s[block, :, cols])
        return carry

    lax.fori_loop(0, d_model // LANES, turn, 0)

    def tables(n, carry):
        rows = aligned(n * LANES, LANES)
        angles = (lax.broadcasted_iota(jnp.int32, (LANES, LANES), 0) + n * LANES).astype(jnp.float32) * freq_ref[...]
        cos_out[rows, :] = jnp.cos(angles) * ROPE_GAIN
        sin_v = jnp.sin(angles) * ROPE_GAIN
        sin_out[rows, :] = jnp.where(first_quarter(angles.shape), -sin_v, sin_v)
        return carry

    lax.fori_loop(0, cos_out.shape[0] // LANES, tables, 0)
    keep_turned = pltpu.make_async_copy(turned_s, turned_out, out_sem.at[1])
    keep_turned.start()
    for copy in gys:
        copy.wait()
    for pair in range(n_pairs - 2, n_pairs):
        keep_qkv(pair).wait()
    keep_turned.wait()
    keep_x.wait()
    own_out.wait()


def enter(hidden, grad_out, gain, freq, w_qkv):
    n_devs, tok, d_model = hidden.shape
    seq, width = n_devs * tok, w_qkv.shape[1]
    anywhere, vmem, dma = pl.BlockSpec(memory_space=pl.ANY), pltpu.VMEM, pltpu.SemaphoreType.DMA
    shape, bf16 = jax.ShapeDtypeStruct, jnp.bfloat16
    local = pl.BlockSpec(memory_space=vmem)
    return pl.pallas_call(
        enter_kernel,
        in_specs=[anywhere, anywhere, local, local, anywhere],
        out_specs=[anywhere] * 4 + [local] * 2,
        out_shape=[shape(hidden.shape, bf16), shape(hidden.shape, bf16), shape((seq, width), jnp.float32), shape((d_model, seq), bf16)]
        + [shape((seq, LANES), jnp.float32)] * 2,
        scratch_shapes=[vmem(hidden.shape, bf16), vmem((tok, d_model), bf16), vmem(w_qkv.shape, bf16), vmem(hidden.shape, bf16),
                        vmem((d_model, seq), bf16), vmem((2, seq, PAIR_W), jnp.float32)]
        + [dma((n_devs,))] * 4 + [dma((4 * width // PAIR_W,)), dma((2,)), dma((2,))],
        compiler_params=pltpu.CompilerParams(vmem_limit_bytes=VMEM_LIMIT, collective_id=2, has_side_effects=True),
        cost_estimate=pl.CostEstimate(flops=COST_FLOPS, bytes_accessed=COST_BYTES, transcendentals=COST_BYTES),
        name="enter",
    )(hidden, grad_out, gain, freq, w_qkv)


def axis_bits():
    me = lax.axis_index('sp')
    coord = {1: lax.rem(me, 2), 2: lax.rem(lax.div(me, 2), 2), 4: lax.div(me, 4)}
    return coord, {bit: {'sp': me + bit * (1 - 2 * coord[bit])} for bit in (1, 2, 4)}


def entry_barrier(peers):
    barrier = pltpu.get_barrier_semaphore()
    for bit in (1, 2, 4):
        pl.semaphore_signal(barrier, inc=1, device_id=peers[bit], device_id_type=MESH)
    pl.semaphore_wait(barrier, 3)


ORDER_OF_HALF = ((2, 4), (4, 2))


def add_rows(dst_ref, a_ref, a_row, b_ref, b_row):
    def body(i, carry):
        step = pl.multiple_of(i * 16, 16)
        total = a_ref[aligned(a_row + step, 16), :] + b_ref[aligned(b_row + step, 16), :].astype(jnp.float32)
        dst_ref[pl.ds(step, 16), :] = total.astype(dst_ref.dtype)
        return carry
    lax.fori_loop(0, dst_ref.shape[0] // 16, body, 0)


class Reduce:
    def __init__(self, coord, peers, sent, own, total, scratch):
        self.coord, self.peers, self.sent, self.own, self.total = coord, peers, sent, own, total
        n = len(sent)
        self.recv_c, self.sum0, self.snd0, self.recv0, self.sum1, self.snd1, self.recv1 = (scratch[k * n:(k + 1) * n] for k in range(7))
        self.send_sem, self.recv_sem = scratch[7 * n:]
        self.n = n

    def copy(self, src, dst, sem, bit):
        return pltpu.make_async_remote_copy(src_ref=src, dst_ref=dst, send_sem=self.send_sem.at[sem], recv_sem=self.recv_sem.at[sem],
                                            device_id=self.peers[bit], device_id_type=MESH)

    def stage_c(self):
        return [self.copy(self.sent[t], self.recv_c[t], t, 1) for t in range(self.n)]

    def stage_s(self, k):
        snd, recv = (self.snd0, self.recv0) if k == 0 else (self.snd1, self.recv1)
        return [self.copy(snd[t].at[h], recv[t].at[h], self.n + 2 * self.n * k + 2 * t + h, ORDER_OF_HALF[h][k])
                for t in range(self.n) for h in range(2)]

    def start(self):
        for copy in self.stage_c():
            copy.start()

    def mid1(self):
        for copy in self.stage_c():
            copy.wait()
        for t in range(self.n):
            half = self.own[t].shape[0] // 2
            for h in range(2):
                c = self.coord[ORDER_OF_HALF[h][0]]
                row = h * half + (1 - c) * (half // 2)
                add_rows(self.snd0[t].at[h], self.own[t], row, self.recv_c[t], row)
        for copy in self.stage_s(0):
            copy.start()
        for t in range(self.n):
            half = self.own[t].shape[0] // 2
            for h in range(2):
                row = h * half + self.coord[ORDER_OF_HALF[h][0]] * (half // 2)
                add_rows(self.sum0[t].at[h], self.own[t], row, self.recv_c[t], row)

    def mid2(self):
        for copy in self.stage_s(0):
            copy.wait()
        for t in range(self.n):
            quarter = self.own[t].shape[0] // 4
            for h in range(2):
                row = (1 - self.coord[ORDER_OF_HALF[h][1]]) * (quarter // 2)
                add_rows(self.snd1[t].at[h], self.sum0[t].at[h], row, self.recv0[t].at[h], row)
        for copy in self.stage_s(1):
            copy.start()
        for t in range(self.n):
            quarter = self.own[t].shape[0] // 4
            for h in range(2):
                row = self.coord[ORDER_OF_HALF[h][1]] * (quarter // 2)
                add_rows(self.sum1[t].at[h], self.sum0[t].at[h], row, self.recv0[t].at[h], row)

    def end(self):
        for copy in self.stage_s(1):
            copy.wait()
        for t in range(self.n):
            for h in range(2):
                add_rows(self.total[t].at[h], self.sum1[t].at[h], 0, self.recv1[t].at[h], 0)

    @staticmethod
    def scratch_shapes(shapes):
        vmem = lambda dtype, div: [pltpu.VMEM((2, r // div, c) if div else (r, c), dtype) for r, c in shapes]
        n = len(shapes)
        return (vmem(jnp.bfloat16, 0) + vmem(jnp.float32, 4) + vmem(jnp.bfloat16, 4) + vmem(jnp.bfloat16, 4)
                + vmem(jnp.float32, 8) + vmem(jnp.bfloat16, 8) + vmem(jnp.bfloat16, 8)
                + [pltpu.SemaphoreType.DMA((5 * n,)), pltpu.SemaphoreType.DMA((5 * n,))])


class Gather:
    def __init__(self, peers, total, pieces, scratch):
        self.peers, self.total, self.pieces = peers, total, pieces
        self.send_sem, self.recv_sem, self.local_sem = scratch
        self.n = len(total)

    def copy(self, src, dst, sem, bit):
        return pltpu.make_async_remote_copy(src_ref=src, dst_ref=dst, send_sem=self.send_sem.at[sem], recv_sem=self.recv_sem.at[sem],
                                            device_id=self.peers[bit], device_id_type=MESH)

    def stage(self, k):
        copies = []
        for t in range(self.n):
            if k == 2:
                copies.append(self.copy(self.pieces[t].at[pl.ds(0, 8)], self.pieces[t].at[pl.ds(8, 8)], 4 * self.n + t, 1))
                continue
            for h in range(2):
                if k == 0:
                    src, dst = self.total[t].at[pl.ds(h, 1)], self.pieces[t].at[pl.ds(4 * h + 1, 1)]
                else:
                    src, dst = self.pieces[t].at[pl.ds(4 * h, 2)], self.pieces[t].at[pl.ds(4 * h + 2, 2)]
                copies.append(self.copy(src, dst, 2 * self.n * k + 2 * t + h, ORDER_OF_HALF[h][1 - k]))
        return copies

    def local(self):
        return [pltpu.make_async_copy(self.total[t].at[pl.ds(h, 1)], self.pieces[t].at[pl.ds(4 * h, 1)], self.local_sem.at[2 * t + h])
                for t in range(self.n) for h in range(2)]

    def start(self):
        for copy in self.stage(0) + self.local():
            copy.start()

    def mid1(self):
        for copy in self.stage(0) + self.local():
            copy.wait()
        for copy in self.stage(1):
            copy.start()

    def mid2(self):
        for copy in self.stage(1):
            copy.wait()
        for copy in self.stage(2):
            copy.start()

    def end(self):
        for copy in self.stage(2):
            copy.wait()

    @staticmethod
    def scratch_shapes(n):
        return [pltpu.SemaphoreType.DMA((5 * n,)), pltpu.SemaphoreType.DMA((5 * n,)), pltpu.SemaphoreType.DMA((2 * n,))]


def attn_kernel(q_ref, k_ref, v_ref, wo_ref, cos_ref, sin_ref, normed_ref, gy_ref,
                o_ref, out_ref, sent_q_out, sent_d_out, own_q_out, own_d_out, total_q_out, total_d_out, pieces_q, pieces_d, *scratch):
    scratch = list(scratch)
    take = lambda n: [scratch.pop(0) for _ in range(n)]
    q_s, do_s, k_var, v_var, k_t, v_t, ot_ref, dq_t, dk_acc, dv_acc = take(10)
    sent, own, total = take(2), take(2), take(2)
    pair = pl.program_id(0)
    coord, peers = axis_bits()
    reduce = Reduce(coord, peers, sent, own, total, take(16))
    chunk = jnp.maximum(pair - 2, 0)
    gather_sems = take(3)
    gather, upcoming = (Gather(peers, total, [ref.at[c] for ref in (pieces_q, pieces_d)], gather_sems)
                        for c in (chunk, lax.rem(pair + pieces_q.shape[0] - 1, pieces_q.shape[0])))
    turn_sem, out_sem = take(2)

    @pl.when(pair == 0)
    def _():
        entry_barrier(peers)

    @pl.when(pair > 0)
    def _():
        for n, bit in enumerate((1, 2, 4)):
            pl.semaphore_signal(turn_sem.at[n], inc=1, device_id=peers[bit], device_id_type=MESH)
        for n in range(3):
            pl.semaphore_wait(turn_sem.at[n], 1)
        reduce.start()

    def middle(first):
        @pl.when(pair > 0)
        def _():
            (reduce.mid1 if first else reduce.mid2)()

        @pl.when(pair > 1)
        def _():
            (gather.mid1 if first else gather.mid2)()

    seq = q_ref.shape[0]
    n_blk = seq // BLK
    half = lax.rem(pair, 2)

    def setup_block(i, carry):
        rows = aligned(i * LANES, LANES)
        cos_v, sin_v = cos_ref[rows, :], sin_ref[rows, :]
        for c in range(2):
            q_s[c, rows, :] = (lane_rotate(q_ref[rows, pl.ds(c * LANES, LANES)], cos_v, sin_v) * 0.125).astype(jnp.bfloat16)
        for vals, var, turned in ((lane_rotate(k_ref[rows, :], cos_v, sin_v), k_var, k_t), (v_ref[rows, :], v_var, v_t)):
            half_variants(vals.astype(jnp.bfloat16).astype(jnp.float32), half, var, turned, rows)
        return carry

    lax.fori_loop(0, seq // LANES, setup_block, 0)

    def grad_attn(n, carry):
        rows = aligned(n * TALL, TALL)
        block = dot_nt(gy_ref[rows, :], wo_ref[...]).astype(jnp.bfloat16)
        do_s[0, rows, :] = block[:, :LANES]
        do_s[1, rows, :] = block[:, LANES:]
        return carry

    lax.fori_loop(0, seq // TALL, grad_attn, 0)
    middle(True)
    dk_acc[...] = jnp.zeros_like(dk_acc)
    dv_acc[...] = jnp.zeros_like(dv_acc)
    low = low_half((BLK, LANES))

    def head_pair(hp, carry):
        for i in range(n_blk):
            rows = pl.ds(i * BLK, BLK)
            q_blk = q_s[hp, rows, :]
            do_blk = do_s[hp, rows, :]
            parts = [(pl.ds(i * BLK, BLK), True)]
            if i:
                parts.append((pl.ds(0, i * BLK), False))
            dv_sum, dk_sum = [0.0] * len(parts), [0.0] * len(parts)
            for par in range(2):
                sub_h = aligned(hp * LANES + par * HEAD, HEAD)
                q_mine = jnp.where(low != par, q_blk, jnp.zeros_like(q_blk))
                do_mine = jnp.where(low != par, do_blk, jnp.zeros_like(do_blk))
                scores, top = [], None
                for keys, is_diag in parts:
                    part = dot_nt(k_var[par, keys, :], q_blk)
                    if is_diag:
                        part = causal_diag(part)
                    scores.append(part)
                    part_top = over_keys(jnp.max, part)
                    top = part_top if top is None else jnp.maximum(top, part_top)
                exps = [jnp.exp(part - top) for part in scores]
                inv = 1.0 / sum(over_keys(jnp.sum, part) for part in exps)
                probs, grads, row_dot, attn = [], [], 0.0, 0.0
                for n, (keys, _) in enumerate(parts):
                    prob = exps[n] * inv
                    prob_b = prob.astype(jnp.bfloat16)
                    grad_p = dot_nt(v_var[par, keys, :], do_blk)
                    row_dot = row_dot + over_keys(jnp.sum, prob * grad_p)
                    attn = attn + dot_nn(v_t[:, keys], prob_b)
                    dv_sum[n] = dv_sum[n] + dot_nn(prob_b, do_mine)
                    probs.append(prob)
                    grads.append(grad_p)
                ot_ref[sub_h, rows] = attn.astype(jnp.bfloat16)
                acc = 0.0
                for n, (keys, _) in enumerate(parts):
                    grad_s = (probs[n] * (grads[n] - row_dot)).astype(jnp.bfloat16)
                    dk_sum[n] = dk_sum[n] + dot_nn(grad_s, q_mine)
                    acc = acc + dot_nn(k_t[:, keys], grad_s)
                dq_t[sub_h, rows] = acc
            for n, (keys, _) in enumerate(parts):
                dv_acc[keys, :] += dv_sum[n]
                dk_acc[keys, :] += dk_sum[n]
        return carry

    lax.fori_loop(0, 2, head_pair, 0)

    def finish_block(i, carry):
        rows = aligned(i * LANES, LANES)
        cos_v, sin_v = cos_ref[rows, :], -sin_ref[rows, :]
        for c in range(2):
            cols = pl.ds(c * LANES, LANES)
            o_ref[rows, cols] = jnp.transpose(ot_ref[cols, rows])
            grad_q = jnp.transpose(dq_t[cols, rows]) * 0.125
            out_ref[rows, cols] = lane_rotate(grad_q, cos_v, sin_v).astype(jnp.bfloat16)
        grad_k, grad_v = (ref[rows, :] + pltpu.roll(ref[rows, :], HEAD, 1) for ref in (dk_acc, dv_acc))
        out_ref[rows, KV_COLS] = jnp.where(low_half(grad_k.shape), lane_rotate(grad_k, cos_v, sin_v), grad_v).astype(jnp.bfloat16)
        return carry

    lax.fori_loop(0, seq // LANES, finish_block, 0)
    mine = coord[1]
    rows_q, rows_d = own[0].shape[0], own[1].shape[0]

    def weight_q(n, carry):
        rows = aligned(n * TALL, TALL)
        for side, ref in ((1 - mine, sent[0]), (mine, own[0])):
            ref[rows, :] = dot_nn(normed_ref[aligned(side * rows_q + n * TALL, TALL), :], out_ref[...]).astype(ref.dtype)
        return carry

    def weight_d(n, carry):
        cols = aligned(n * BLK, BLK)
        both = dot_nn(ot_ref[...], gy_ref[:, cols])
        top, bottom = both[:rows_d], both[rows_d:]
        own[1][:, cols] = jnp.where(mine == 0, top, bottom)
        sent[1][:, cols] = jnp.where(mine == 0, bottom, top).astype(jnp.bfloat16)
        return carry

    middle(False)
    lax.fori_loop(0, rows_q // TALL, weight_q, 0)
    lax.fori_loop(0, gy_ref.shape[1] // BLK, weight_d, 0)

    @pl.when(pair > 0)
    def _():
        reduce.end()

    @pl.when(pair > 1)
    def _():
        gather.end()

    @pl.when(jnp.logical_and(pair > 0, pair < pl.num_programs(0) - 1))
    def _():
        upcoming.start()

    @pl.when(pair == pl.num_programs(0) - 1)
    def _():
        outs = [sent_q_out, sent_d_out, own_q_out, own_d_out, total_q_out, total_d_out]
        copies = [pltpu.make_async_copy(src, dst, out_sem.at[n]) for n, (src, dst) in enumerate(zip(sent + own + total, outs))]
        for copy in copies:
            copy.start()
        for copy in copies:
            copy.wait()


def total_shapes(own):
    return [jax.ShapeDtypeStruct((2, o.shape[0] // 8, o.shape[1]), jnp.bfloat16) for o in own]


def piece_shapes(total):
    return [jax.ShapeDtypeStruct((16,) + t.shape[1:], jnp.bfloat16) for t in total]


def attention(qkv, w_o, cos_t, sin_t, normed_t, grad_y):
    seq, d_model = grad_y.shape
    n_steps = qkv.shape[1] // GROUP_W
    const = lambda shape: pl.BlockSpec(shape, lambda p: (0,) * len(shape), pipeline_mode=pl.Buffered(1))
    col = lambda width: pl.BlockSpec((seq, width), lambda p: (0, p))
    of_pair = lambda at: pl.BlockSpec((seq, LANES), lambda p: (0, p // 2 * (PAIR_W // LANES) + at))
    anywhere = pl.BlockSpec(memory_space=pl.ANY)
    shape = jax.ShapeDtypeStruct
    slab = pltpu.VMEM((2, seq, LANES), jnp.bfloat16)
    turned = pltpu.VMEM((HEAD, seq), jnp.bfloat16)
    acc = pltpu.VMEM((seq, LANES), jnp.float32)
    partial = [(d_model // 2, GROUP_W), (Q_COLS // 2, d_model)]
    own = [shape(p, jnp.float32) for p in partial]
    sent = [shape(p, jnp.bfloat16) for p in partial]
    totals = total_shapes(own)
    pieces = [shape((n_steps - 2,) + p.shape, p.dtype) for p in piece_shapes(totals)]
    kept = [pltpu.VMEM(p.shape, p.dtype) for p in sent + own + totals]
    out = pl.pallas_call(
        attn_kernel,
        grid=(n_steps,),
        in_specs=[pl.BlockSpec((seq, Q_COLS), lambda p: (0, p // 2 * (PAIR_W // Q_COLS) + p % 2)), of_pair(4), of_pair(5), pl.BlockSpec((Q_COLS, d_model), lambda p: (p, 0)), const((seq, LANES)), const((seq, LANES)), const((d_model, seq)), const((seq, d_model))],
        out_specs=[col(Q_COLS), col(GROUP_W)] + [anywhere] * 8,
        out_shape=[shape((seq, Q_COLS * n_steps), jnp.bfloat16), shape((seq, GROUP_W * n_steps), jnp.bfloat16)] + sent + own + totals + pieces,
        scratch_shapes=[slab, slab, slab, slab, turned, turned, pltpu.VMEM((Q_COLS, seq), jnp.bfloat16), pltpu.VMEM((Q_COLS, seq), jnp.float32), acc, acc]
        + kept + Reduce.scratch_shapes(partial) + Gather.scratch_shapes(2)
        + [pltpu.SemaphoreType.REGULAR((3,)), pltpu.SemaphoreType.DMA((6,))],
        compiler_params=pltpu.CompilerParams(vmem_limit_bytes=VMEM_LIMIT, collective_id=0, has_side_effects=True),
        cost_estimate=pl.CostEstimate(flops=COST_FLOPS, bytes_accessed=COST_BYTES, transcendentals=COST_BYTES),
        name="attn",
    )(qkv, qkv, qkv, w_o, cos_t, sin_t, normed_t, grad_y)
    return out[0], out[1], (list(out[2:4]), list(out[4:6])), list(out[6:8]), out[8:10]


def finish_kernel(o_ref, x_ref, grads_ref, gy_ref, gain_ref, wo_ref, w_hbm, sent_q, sent_d, own_q, own_d, old_q, old_d,
                  y_out, gh_out, old_pieces_q, old_pieces_d, pieces_q, pieces_d, norm_out, *scratch):
    scratch = list(scratch)
    take = lambda n: [scratch.pop(0) for _ in range(n)]
    y_s, gh_s, w_s, dh_s, norm_ref, norm_row, norm_all = take(7)
    total = take(2)
    step = pl.program_id(0)
    me = lax.axis_index('sp')
    coord, peers = axis_bits()
    reduce = Reduce(coord, peers, [sent_q, sent_d], [own_q, own_d], total, take(16))
    gather = Gather(peers, [old_q, old_d], [old_pieces_q, old_pieces_d], take(3))
    last = Gather(peers, total, [pieces_q, pieces_d], take(3))
    w_sem, y_send, y_recv, gh_send, gh_recv, norm_send, norm_recv = take(7)
    n_devs = y_out.shape[0]
    tok = y_out.shape[1]
    half_steps = pl.num_programs(0) // 2
    per_step = n_devs // half_steps
    weights = load_weights(w_hbm, w_s, w_sem, (0, GROUP_W, Q_COLS, PAIR_W - LANES))

    def share(values, out, send_sem, recv_sem, dest, act):
        @pl.when(dest == me)
        def _():
            act(pltpu.make_async_copy(values.at[dest], out.at[dest], send_sem.at[dest]), True)

        @pl.when(dest != me)
        def _():
            act(pltpu.make_async_remote_copy(src_ref=values.at[dest], dst_ref=out.at[me], send_sem=send_sem.at[dest], recv_sem=recv_sem.at[me],
                                             device_id={'sp': dest}, device_id_type=MESH), False)

    def send(values, out, send_sem, recv_sem, dests):
        for dest in dests:
            share(values, out, send_sem, recv_sem, dest, lambda copy, local: copy.start())

    def finish(values, out, send_sem, recv_sem):
        for peer in range(n_devs):
            @pl.when(peer == me)
            def _():
                pltpu.make_async_copy(values.at[peer], out.at[peer], send_sem.at[peer]).wait()

            @pl.when(peer != me)
            def _():
                pltpu.make_async_remote_copy(src_ref=values.at[peer], dst_ref=out.at[peer], send_sem=send_sem.at[peer], recv_sem=recv_sem.at[peer],
                                             device_id={'sp': peer}, device_id_type=MESH).wait()

    def share_norm(act):
        for k in range(1, n_devs):
            peer = lax.rem(me + k, n_devs)
            copy = pltpu.make_async_remote_copy(src_ref=norm_row, dst_ref=norm_all.at[me], send_sem=norm_send.at[k], recv_sem=norm_recv.at[k],
                                                device_id={'sp': peer}, device_id_type=MESH)
            act(copy)

    @pl.when(step == 0)
    def _():
        greet_all(me, n_devs)
        reduce.start()
        gather.start()
        for copy in weights:
            copy.start()
        norm_ref[...] = jnp.zeros_like(norm_ref)

    @pl.when(step == 1)
    def _():
        reduce.mid1()
        gather.mid1()

    @pl.when(jnp.logical_and(step >= 1, step <= half_steps))
    def _():
        send(y_s, y_out, y_send, y_recv, [(step - 1) * per_step + k for k in range(per_step)])

    d_model = wo_ref.shape[1]

    @pl.when(step < half_steps)
    def _():
        def cols_of_y(n, carry):
            cols = aligned(n * 512, 512)
            block = (x_ref[:, cols].astype(jnp.float32) + dot_nn(o_ref[...], wo_ref[:, cols])).astype(jnp.bfloat16)
            for k in range(per_step):
                y_s[step * per_step + k, :, cols] = block[k * tok:(k + 1) * tok, :]
            return carry
        lax.fori_loop(0, d_model // 512, cols_of_y, 0)

    @pl.when(step == half_steps)
    def _():
        for copy in weights:
            copy.wait()

        def pair_up(n, carry):
            rows = aligned(n * LANES, LANES)
            for pair in range(w_s.shape[1] // PAIR_W):
                spots = [pl.ds(pair * PAIR_W + at, LANES) for at in (Q_COLS, PAIR_W - LANES)]
                for spot, cols in zip(spots, cross(*[w_s[rows, spot].astype(jnp.float32) for spot in spots])):
                    w_s[rows, spot] = cols.astype(jnp.bfloat16)
            return carry

        lax.fori_loop(0, d_model // LANES, pair_up, 0)

    @pl.when(step >= half_steps)
    def _():
        def cols_of_dh(n, carry):
            rows = aligned(n * 512, 512)
            dh_s[:, rows] = dot_nt(grads_ref[...], w_s[rows, :])
            return carry
        lax.fori_loop(0, d_model // 512, cols_of_dh, 0)
        gain = gain_ref[...]

        def norm_rows(n, carry):
            rows = aligned(n * 16, 16)
            x_f = x_ref[rows, :].astype(jnp.float32)
            inv_rms = lax.rsqrt(jnp.mean(x_f * x_f, axis=-1, keepdims=True) + NORM_EPS)
            unit = x_f * inv_rms
            grad_normed = dh_s[rows, :]
            grad_unit = grad_normed * gain
            mean_dot = jnp.mean(grad_unit * unit, axis=-1, keepdims=True)
            grad_x = gy_ref[rows, :].astype(jnp.float32) + inv_rms * (grad_unit - unit * mean_dot)
            place = (step - half_steps) * per_step + n // (tok // 16)
            gh_s[place, aligned(lax.rem(n, tok // 16) * 16, 16), :] = grad_x.astype(jnp.bfloat16)
            weighted = grad_normed * unit
            norm_ref[...] += weighted[:8, :] + weighted[8:, :]
            return carry
        lax.fori_loop(0, per_step * tok // 16, norm_rows, 0)

    @pl.when(step == pl.num_programs(0) - 1)
    def _():
        gh = (gh_s, gh_out, gh_send, gh_recv)
        norm_row[...] = over_keys(jnp.sum, norm_ref[...])
        reduce.mid2()
        gather.mid2()
        share_norm(lambda copy: copy.start())
        send(*gh, range(n_devs // 2))
        reduce.end()
        last.start()
        send(*gh, range(n_devs // 2, n_devs))
        gather.end()
        last.mid1()
        last.mid2()
        share_norm(lambda copy: copy.wait())
        norm_all[me] = norm_row[...]
        norm_out[...] = sum(norm_all[peer] for peer in range(n_devs))
        finish(y_s, y_out, y_send, y_recv)
        last.end()
        finish(*gh)


def finish(attn, x, grads, grad_y, gain, w_o, w_qkv, reduce, old_total, n_devs):
    seq, d_model = x.shape
    sent, own = reduce
    steps = 8
    rows = 2 * seq // steps
    tok = seq // n_devs
    const = lambda shape: pl.BlockSpec(shape, lambda s: (0,) * len(shape), pipeline_mode=pl.Buffered(1))
    early = lambda width: pl.BlockSpec((rows, width), lambda s: (jnp.minimum(s, steps // 2 - 1), 0))
    late = lambda width: pl.BlockSpec((rows, width), lambda s: (jnp.maximum(s - steps // 2, 0), 0))
    anywhere = pl.BlockSpec(memory_space=pl.ANY)
    shape = jax.ShapeDtypeStruct
    totals = total_shapes(own)
    tokens = shape((n_devs, tok, d_model), jnp.bfloat16)
    dma = lambda: pltpu.SemaphoreType.DMA((n_devs,))
    out = pl.pallas_call(
        finish_kernel,
        grid=(steps,),
        in_specs=[early(q_w) for q_w in (attn.shape[1],)] + [pl.BlockSpec((rows, d_model), lambda s: (lax.rem(s, steps // 2), 0)), late(grads.shape[1]), late(d_model),
                  const((1, d_model)), const(w_o.shape), anywhere, anywhere, anywhere]
        + [const(o.shape) for o in own] + [const(t.shape) for t in totals],
        out_specs=[anywhere] * 6 + [pl.BlockSpec((1, d_model), lambda s: (0, 0))],
        out_shape=[tokens, tokens] + piece_shapes(totals) + piece_shapes(totals) + [shape((1, d_model), jnp.float32)],
        scratch_shapes=[pltpu.VMEM(tokens.shape, jnp.bfloat16), pltpu.VMEM(tokens.shape, jnp.bfloat16),
                        pltpu.VMEM(w_qkv.shape, jnp.bfloat16), pltpu.VMEM((rows, d_model), jnp.float32),
                        pltpu.VMEM((8, d_model), jnp.float32), pltpu.VMEM((1, d_model), jnp.float32),
                        pltpu.VMEM((n_devs, 1, d_model), jnp.float32)]
        + [pltpu.VMEM(t.shape, t.dtype) for t in totals]
        + Reduce.scratch_shapes([o.shape for o in own]) + Gather.scratch_shapes(2) + Gather.scratch_shapes(2)
        + [pltpu.SemaphoreType.DMA((4 * w_qkv.shape[1] // PAIR_W,))] + [dma()] * 6,
        compiler_params=pltpu.CompilerParams(vmem_limit_bytes=VMEM_LIMIT, collective_id=1, has_side_effects=True),
        cost_estimate=pl.CostEstimate(flops=COST_FLOPS, bytes_accessed=COST_BYTES, transcendentals=COST_BYTES),
        name="finish",
    )(attn, x, grads, grad_y, gain, w_o, w_qkv, *sent, *own, *old_total)
    return out[0], out[1], out[2:4], out[4:6], out[6]


def place_kernel(n, slots, *refs):
    pieces_q, pieces_d, tokens = refs[:n], refs[n:2 * n], refs[2 * n:2 * n + 2]
    q_out, d_out, *tokens_out = refs[2 * n + 2:]
    for src, dst in zip(tokens, tokens_out):
        dst[...] = src[...]
    for c in range(n):
        d_out[c] = pieces_d[c][0, 0].astype(jnp.float32)
        q_out[:, pl.ds(c * Q_COLS, Q_COLS)] = pieces_q[c][0, 0, :, :Q_COLS].astype(jnp.float32)
    for pair in range(n // 2):
        grads = cross(*[ref[0, 0, :, Q_COLS:].astype(jnp.float32) for ref in pieces_q[2 * pair:2 * pair + 2]])
        for at, grad in zip((n * Q_COLS, q_out.shape[1] - n * HEAD), grads):
            q_out[:, pl.ds(at + pair * LANES, LANES)] = grad


def place(slots, parts_q, parts_d, tokens):
    specs, args, sizes = [], [], []
    for parts in (parts_q, parts_d):
        chunks = [(part, c) for part in parts for c in range(part.shape[0])]
        rows, width = parts[0].shape[2:]
        specs += [pl.BlockSpec((1, 1, rows, width), lambda s, slots, c=c: (c, s, 0, 0)) for _, c in chunks]
        args += [part for part, _ in chunks]
        sizes.append((len(chunks), rows, width))
    (n_pairs, rows_q, width_q), (_, rows_d, width_d) = sizes
    flat = [t.reshape(16, -1, t.shape[-1]) for t in tokens]
    through = pl.BlockSpec((1,) + flat[0].shape[1:], lambda s, slots: (s, 0, 0))
    shape = jax.ShapeDtypeStruct
    grad_q, grad_d, *out = pl.pallas_call(
        functools.partial(place_kernel, n_pairs),
        grid_spec=pltpu.PrefetchScalarGridSpec(
            num_scalar_prefetch=1, grid=(16,), in_specs=specs + [through] * 2,
            out_specs=[pl.BlockSpec((rows_q, n_pairs * width_q), lambda s, slots: (slots[s], 0)),
                       pl.BlockSpec((n_pairs, rows_d, width_d), lambda s, slots: (0, slots[s], 0)), through, through]),
        out_shape=[shape((16 * rows_q, n_pairs * width_q), jnp.float32), shape((n_pairs, 16 * rows_d, width_d), jnp.float32)]
        + [shape(t.shape, t.dtype) for t in flat],
        compiler_params=pltpu.CompilerParams(vmem_limit_bytes=VMEM_LIMIT),
        cost_estimate=pl.CostEstimate(flops=COST_FLOPS, bytes_accessed=COST_BYTES, transcendentals=COST_BYTES),
        name="place",
    )(slots, *args, *flat)
    return grad_q, grad_d, [o.reshape(t.shape) for o, t in zip(out, tokens)]


def row_slots():
    me = lax.axis_index('sp')
    core, x, y = me & 1, (me >> 1) & 1, me >> 2
    order = []
    for c in (core, 1 - core):
        for half, (a, b) in enumerate(((x, y), (y, x))):
            for a_i in (a, 1 - a):
                for b_i in (b, 1 - b):
                    order.append(c * 8 + half * 4 + a_i * 2 + b_i)
    return jnp.stack(order).astype(jnp.int32)


def solution(mesh):
    n_devs = mesh.shape['sp']

    def device_step(hidden, norm_w, w_qkv, w_out, long_factor, grad_out):
        d_model = hidden.shape[-1]
        gain = norm_w.astype(jnp.float32)[None]
        x, grad_y, qkv, normed_t, cos_t, sin_t = enter(hidden, grad_out, gain, inverse_frequencies(long_factor), w_qkv)
        x, grad_y = x.reshape(-1, d_model), grad_y.reshape(-1, d_model)
        w_o = w_out.reshape(-1, d_model)
        attn, grads, partial, total, pieces = attention(qkv, w_o, cos_t, sin_t, normed_t, grad_y)
        block_out, grad_hidden, before_last, last, grad_norm_w = finish(attn, x, grads, grad_y, gain, w_o, w_qkv, partial, total, n_devs)
        parts = [[first, second[None], third[None]] for first, second, third in zip(pieces, before_last, last)]
        grad_w_qkv, grad_w_out, (block_out, grad_hidden) = place(row_slots(), *parts, (block_out, grad_hidden))
        return block_out, grad_hidden, grad_w_qkv, grad_w_out.reshape(w_out.shape), grad_norm_w.reshape(-1)

    tok_spec = P('dp', 'sp', None)
    return jax.shard_map(device_step, mesh=mesh,
                         in_specs=(tok_spec, P(), P(), P(), P(), tok_spec),
                         out_specs=(tok_spec, tok_spec, P('dp', None), P('dp', None, None), P('dp')),
                         check_vma=False)
```

```python
import functools
import math
import jax
import jax.numpy as jnp
from jax import lax
from jax.experimental import pallas as pl
from jax.experimental.pallas import tpu as pltpu
from jax.sharding import PartitionSpec as P

NORM_EPS = 1e-5
ROPE_BASE = 10000.0
ROPE_GAIN = math.sqrt(1.0 + math.log(32.0) / math.log(4096.0))
MASK_VALUE = -1e30
BLK = 256
TALL = 512
LANES = 128
HEAD = LANES // 2
Q_COLS = 2 * LANES
GROUP_W = Q_COLS + LANES
PAIR_W = 2 * GROUP_W
KV_COLS = pl.ds(Q_COLS, LANES)
MESH = pl.DeviceIdType.MESH
VMEM_LIMIT = 67_000_000
COST_BYTES = 2**26
COST_FLOPS = 10**11


def inverse_frequencies(long_factor):
    half_rot = long_factor.shape[0]
    exponent = jnp.arange(half_rot, dtype=jnp.float32) / half_rot
    inv_freq = 1.0 / (long_factor * jnp.power(ROPE_BASE, exponent))
    return jnp.tile(inv_freq, LANES // half_rot)[None]


def first_quarter(shape):
    return lax.broadcasted_iota(jnp.int32, shape, 1) % HEAD < HEAD // 2


def lane_rotate(vals, cos_v, sin_v):
    first = first_quarter(vals.shape)
    partner = jnp.where(first, pltpu.roll(vals, LANES - 32, 1), pltpu.roll(vals, 32, 1))
    return vals * cos_v + partner * sin_v


def low_half(shape):
    return lax.broadcasted_iota(jnp.int32, shape, 1) < HEAD


def cross(a, b):
    low = low_half(a.shape)
    return jnp.where(low, a, pltpu.roll(b, HEAD, 1)), jnp.where(low, pltpu.roll(a, HEAD, 1), b)


def half_variants(vals, half, out_ref, turned_ref, rows):
    low = low_half(vals.shape)
    swapped = pltpu.roll(vals, HEAD, 1)
    first, second = jnp.where(half == 0, vals, swapped), jnp.where(half == 0, swapped, vals)
    out_ref[0, rows, :] = jnp.where(low, first, 0.0).astype(jnp.bfloat16)
    out_ref[1, rows, :] = jnp.where(low, 0.0, second).astype(jnp.bfloat16)
    turned_ref[:, rows] = jnp.transpose(first)[:HEAD].astype(jnp.bfloat16)


def over_keys(reduce, vals):
    return reduce(vals, axis=0, keepdims=True)


def aligned(start, size):
    return pl.ds(pl.multiple_of(start, size), size)


def dot_nt(a, b):
    return lax.dot_general(a, b, (((1,), (1,)), ((), ())), preferred_element_type=jnp.float32)


def dot_nn(a, b):
    return lax.dot_general(a, b, (((1,), (0,)), ((), ())), preferred_element_type=jnp.float32)


def causal_diag(scores):
    keys = lax.broadcasted_iota(jnp.int32, scores.shape, 0)
    rows = lax.broadcasted_iota(jnp.int32, scores.shape, 1)
    return jnp.where(keys <= rows, scores, MASK_VALUE)


def load_weights(w_hbm, w_s, sem, places):
    width = w_hbm.shape[1]
    n_pairs = width // PAIR_W
    copies = []
    for pair in range(n_pairs):
        q, k, v = pair * 2 * Q_COLS, n_pairs * 2 * Q_COLS + pair * LANES, width - (n_pairs - pair) * LANES
        for src, cols, dst in zip((q, q + Q_COLS, k, v), (Q_COLS, Q_COLS, LANES, LANES), places):
            copies.append(pltpu.make_async_copy(w_hbm.at[:, pl.ds(src, cols)], w_s.at[:, pl.ds(pair * PAIR_W + dst, cols)], sem.at[len(copies)]))
    return copies


def greet_all(me, n_devs):
    barrier = pltpu.get_barrier_semaphore()
    for k in range(1, n_devs):
        pl.semaphore_signal(barrier, inc=1, device_id={'sp': lax.rem(me + k, n_devs)}, device_id_type=MESH)
    pl.semaphore_wait(barrier, n_devs - 1)


def enter_kernel(hidden, grad_out, gain_ref, freq_ref, w_hbm, x_out, gy_out, qkv_out, turned_out, cos_out, sin_out, x_s, own_s, w_s, h_s, turned_s, stage,
                 x_send, x_recv, gy_send, gy_recv, w_sem, out_sem, stage_sem):
    n_devs, tok, d_model = hidden.shape
    me = lax.axis_index('sp')

    def to_peer(src, dst, send_sem, recv_sem, k):
        peer = lax.rem(me + k, n_devs)
        return pltpu.make_async_remote_copy(src_ref=src.at[peer], dst_ref=dst.at[me], send_sem=send_sem.at[k], recv_sem=recv_sem.at[k],
                                            device_id={'sp': peer}, device_id_type=MESH)

    weights = load_weights(w_hbm, w_s, w_sem, (0, Q_COLS, 2 * Q_COLS, PAIR_W - LANES))
    own_x = pltpu.make_async_copy(hidden.at[me], x_s.at[me], x_send.at[0])
    own_in = pltpu.make_async_copy(grad_out.at[me], own_s, gy_send.at[0])
    own_out = pltpu.make_async_copy(own_s, gy_out.at[me], gy_recv.at[0])
    greet_all(me, n_devs)
    peers = range(1, n_devs)
    xs = [to_peer(hidden, x_s, x_send, x_recv, k) for k in peers]
    gys = [to_peer(grad_out, gy_out, gy_send, gy_recv, k) for k in peers]
    for copy in xs + gys + [own_x, own_in] + weights:
        copy.start()
    gain = gain_ref[...]

    def norm_block(block):
        def norm_rows(n, carry):
            rows = aligned(n * 16, 16)
            x_f = x_s[block, rows, :].astype(jnp.float32)
            inv_rms = lax.rsqrt(jnp.mean(x_f * x_f, axis=-1, keepdims=True) + NORM_EPS)
            h_s[block, rows, :] = (x_f * inv_rms * gain).astype(jnp.bfloat16)
            return carry
        lax.fori_loop(0, tok // 16, norm_rows, 0)

    own_x.wait()
    norm_block(me)
    for k, copy in zip(peers, xs):
        copy.wait()
        norm_block(lax.rem(me + n_devs - k, n_devs))
    own_in.wait()
    own_out.start()
    for copy in weights:
        copy.wait()
    keep_x = pltpu.make_async_copy(x_s, x_out, out_sem.at[0])
    keep_x.start()

    def keep_qkv(pair):
        return pltpu.make_async_copy(stage.at[pair % 2], qkv_out.at[:, pl.ds(pair * PAIR_W, PAIR_W)], stage_sem.at[pair % 2])

    half = n_devs // 2
    n_pairs = w_hbm.shape[1] // PAIR_W
    for pair in range(n_pairs):
        if pair > 1:
            keep_qkv(pair - 2).wait()

        def columns(n, carry):
            for m in range(2):
                left = h_s[pl.ds(m * half, half)].reshape(half * tok, d_model)
                stage[pair % 2, pl.ds(m * half * tok, half * tok), aligned(n * BLK, BLK)] = dot_nn(left, w_s[:, aligned(pair * PAIR_W + n * BLK, BLK)])
            return carry

        lax.fori_loop(0, PAIR_W // BLK, columns, 0)
        keep_qkv(pair).start()

    def turn(n, carry):
        cols = aligned(n * LANES, LANES)
        for block in range(n_devs):
            turned_s[cols, pl.ds(block * tok, tok)] = jnp.transpose(h_s[block, :, cols])
        return carry

    lax.fori_loop(0, d_model // LANES, turn, 0)

    def tables(n, carry):
        rows = aligned(n * LANES, LANES)
        angles = (lax.broadcasted_iota(jnp.int32, (LANES, LANES), 0) + n * LANES).astype(jnp.float32) * freq_ref[...]
        cos_out[rows, :] = jnp.cos(angles) * ROPE_GAIN
        sin_v = jnp.sin(angles) * ROPE_GAIN
        sin_out[rows, :] = jnp.where(first_quarter(angles.shape), -sin_v, sin_v)
        return carry

    lax.fori_loop(0, cos_out.shape[0] // LANES, tables, 0)
    keep_turned = pltpu.make_async_copy(turned_s, turned_out, out_sem.at[1])
    keep_turned.start()
    for copy in gys:
        copy.wait()
    for pair in range(n_pairs - 2, n_pairs):
        keep_qkv(pair).wait()
    keep_turned.wait()
    keep_x.wait()
    own_out.wait()


def enter(hidden, grad_out, gain, freq, w_qkv):
    n_devs, tok, d_model = hidden.shape
    seq, width = n_devs * tok, w_qkv.shape[1]
    anywhere, vmem, dma = pl.BlockSpec(memory_space=pl.ANY), pltpu.VMEM, pltpu.SemaphoreType.DMA
    shape, bf16 = jax.ShapeDtypeStruct, jnp.bfloat16
    local = pl.BlockSpec(memory_space=vmem)
    return pl.pallas_call(
        enter_kernel,
        in_specs=[anywhere, anywhere, local, local, anywhere],
        out_specs=[anywhere] * 4 + [local] * 2,
        out_shape=[shape(hidden.shape, bf16), shape(hidden.shape, bf16), shape((seq, width), jnp.float32), shape((d_model, seq), bf16)]
        + [shape((seq, LANES), jnp.float32)] * 2,
        scratch_shapes=[vmem(hidden.shape, bf16), vmem((tok, d_model), bf16), vmem(w_qkv.shape, bf16), vmem(hidden.shape, bf16),
                        vmem((d_model, seq), bf16), vmem((2, seq, PAIR_W), jnp.float32)]
        + [dma((n_devs,))] * 4 + [dma((4 * width // PAIR_W,)), dma((2,)), dma((2,))],
        compiler_params=pltpu.CompilerParams(vmem_limit_bytes=VMEM_LIMIT, collective_id=2, has_side_effects=True),
        cost_estimate=pl.CostEstimate(flops=COST_FLOPS, bytes_accessed=COST_BYTES, transcendentals=COST_BYTES),
        name="enter",
    )(hidden, grad_out, gain, freq, w_qkv)


def axis_bits():
    me = lax.axis_index('sp')
    coord = {1: lax.rem(me, 2), 2: lax.rem(lax.div(me, 2), 2), 4: lax.div(me, 4)}
    return coord, {bit: {'sp': me + bit * (1 - 2 * coord[bit])} for bit in (1, 2, 4)}


def entry_barrier(peers):
    barrier = pltpu.get_barrier_semaphore()
    for bit in (1, 2, 4):
        pl.semaphore_signal(barrier, inc=1, device_id=peers[bit], device_id_type=MESH)
    pl.semaphore_wait(barrier, 3)


ORDER_OF_HALF = ((2, 4), (4, 2))


def add_rows(dst_ref, a_ref, a_row, b_ref, b_row):
    def body(i, carry):
        step = pl.multiple_of(i * 16, 16)
        total = a_ref[aligned(a_row + step, 16), :] + b_ref[aligned(b_row + step, 16), :].astype(jnp.float32)
        dst_ref[pl.ds(step, 16), :] = total.astype(dst_ref.dtype)
        return carry
    lax.fori_loop(0, dst_ref.shape[0] // 16, body, 0)


class Reduce:
    def __init__(self, coord, peers, sent, own, total, scratch):
        self.coord, self.peers, self.sent, self.own, self.total = coord, peers, sent, own, total
        n = len(sent)
        self.recv_c, self.sum0, self.snd0, self.recv0, self.sum1, self.snd1, self.recv1 = (scratch[k * n:(k + 1) * n] for k in range(7))
        self.send_sem, self.recv_sem = scratch[7 * n:]
        self.n = n

    def copy(self, src, dst, sem, bit):
        return pltpu.make_async_remote_copy(src_ref=src, dst_ref=dst, send_sem=self.send_sem.at[sem], recv_sem=self.recv_sem.at[sem],
                                            device_id=self.peers[bit], device_id_type=MESH)

    def stage_c(self):
        return [self.copy(self.sent[t], self.recv_c[t], t, 1) for t in range(self.n)]

    def stage_s(self, k):
        snd, recv = (self.snd0, self.recv0) if k == 0 else (self.snd1, self.recv1)
        return [self.copy(snd[t].at[h], recv[t].at[h], self.n + 2 * self.n * k + 2 * t + h, ORDER_OF_HALF[h][k])
                for t in range(self.n) for h in range(2)]

    def start(self):
        for copy in self.stage_c():
            copy.start()

    def mid1(self):
        for copy in self.stage_c():
            copy.wait()
        for t in range(self.n):
            half = self.own[t].shape[0] // 2
            for h in range(2):
                c = self.coord[ORDER_OF_HALF[h][0]]
                row = h * half + (1 - c) * (half // 2)
                add_rows(self.snd0[t].at[h], self.own[t], row, self.recv_c[t], row)
        for copy in self.stage_s(0):
            copy.start()
        for t in range(self.n):
            half = self.own[t].shape[0] // 2
            for h in range(2):
                row = h * half + self.coord[ORDER_OF_HALF[h][0]] * (half // 2)
                add_rows(self.sum0[t].at[h], self.own[t], row, self.recv_c[t], row)

    def mid2(self):
        for copy in self.stage_s(0):
            copy.wait()
        for t in range(self.n):
            quarter = self.own[t].shape[0] // 4
            for h in range(2):
                row = (1 - self.coord[ORDER_OF_HALF[h][1]]) * (quarter // 2)
                add_rows(self.snd1[t].at[h], self.sum0[t].at[h], row, self.recv0[t].at[h], row)
        for copy in self.stage_s(1):
            copy.start()
        for t in range(self.n):
            quarter = self.own[t].shape[0] // 4
            for h in range(2):
                row = self.coord[ORDER_OF_HALF[h][1]] * (quarter // 2)
                add_rows(self.sum1[t].at[h], self.sum0[t].at[h], row, self.recv0[t].at[h], row)

    def end(self):
        for copy in self.stage_s(1):
            copy.wait()
        for t in range(self.n):
            for h in range(2):
                add_rows(self.total[t].at[h], self.sum1[t].at[h], 0, self.recv1[t].at[h], 0)

    @staticmethod
    def scratch_shapes(shapes):
        vmem = lambda dtype, div: [pltpu.VMEM((2, r // div, c) if div else (r, c), dtype) for r, c in shapes]
        n = len(shapes)
        return (vmem(jnp.bfloat16, 0) + vmem(jnp.float32, 4) + vmem(jnp.bfloat16, 4) + vmem(jnp.bfloat16, 4)
                + vmem(jnp.float32, 8) + vmem(jnp.bfloat16, 8) + vmem(jnp.bfloat16, 8)
                + [pltpu.SemaphoreType.DMA((5 * n,)), pltpu.SemaphoreType.DMA((5 * n,))])


class Gather:
    def __init__(self, peers, total, pieces, scratch):
        self.peers, self.total, self.pieces = peers, total, pieces
        self.send_sem, self.recv_sem, self.local_sem = scratch
        self.n = len(total)

    def copy(self, src, dst, sem, bit):
        return pltpu.make_async_remote_copy(src_ref=src, dst_ref=dst, send_sem=self.send_sem.at[sem], recv_sem=self.recv_sem.at[sem],
                                            device_id=self.peers[bit], device_id_type=MESH)

    def stage(self, k):
        copies = []
        for t in range(self.n):
            if k == 2:
                copies.append(self.copy(self.pieces[t].at[pl.ds(0, 8)], self.pieces[t].at[pl.ds(8, 8)], 4 * self.n + t, 1))
                continue
            for h in range(2):
                if k == 0:
                    src, dst = self.total[t].at[pl.ds(h, 1)], self.pieces[t].at[pl.ds(4 * h + 1, 1)]
                else:
                    src, dst = self.pieces[t].at[pl.ds(4 * h, 2)], self.pieces[t].at[pl.ds(4 * h + 2, 2)]
                copies.append(self.copy(src, dst, 2 * self.n * k + 2 * t + h, ORDER_OF_HALF[h][1 - k]))
        return copies

    def local(self):
        return [pltpu.make_async_copy(self.total[t].at[pl.ds(h, 1)], self.pieces[t].at[pl.ds(4 * h, 1)], self.local_sem.at[2 * t + h])
                for t in range(self.n) for h in range(2)]

    def start(self):
        for copy in self.stage(0) + self.local():
            copy.start()

    def mid1(self):
        for copy in self.stage(0) + self.local():
            copy.wait()
        for copy in self.stage(1):
            copy.start()

    def mid2(self):
        for copy in self.stage(1):
            copy.wait()
        for copy in self.stage(2):
            copy.start()

    def end(self):
        for copy in self.stage(2):
            copy.wait()

    @staticmethod
    def scratch_shapes(n):
        return [pltpu.SemaphoreType.DMA((5 * n,)), pltpu.SemaphoreType.DMA((5 * n,)), pltpu.SemaphoreType.DMA((2 * n,))]


def attn_kernel(q_ref, k_ref, v_ref, wo_ref, cos_ref, sin_ref, normed_ref, gy_ref,
                o_ref, out_ref, sent_q_out, sent_d_out, own_q_out, own_d_out, total_q_out, total_d_out, pieces_q, pieces_d, *scratch):
    scratch = list(scratch)
    take = lambda n: [scratch.pop(0) for _ in range(n)]
    q_s, do_s, k_var, v_var, k_t, v_t, ot_ref, dq_t, dk_acc, dv_acc = take(10)
    sent, own, total = take(2), take(2), take(2)
    pair = pl.program_id(0)
    coord, peers = axis_bits()
    reduce = Reduce(coord, peers, sent, own, total, take(16))
    chunk = jnp.maximum(pair - 2, 0)
    gather_sems = take(3)
    gather, upcoming = (Gather(peers, total, [ref.at[c] for ref in (pieces_q, pieces_d)], gather_sems)
                        for c in (chunk, lax.rem(pair + pieces_q.shape[0] - 1, pieces_q.shape[0])))
    turn_sem, out_sem = take(2)

    @pl.when(pair == 0)
    def _():
        entry_barrier(peers)

    @pl.when(pair > 0)
    def _():
        for n, bit in enumerate((1, 2, 4)):
            pl.semaphore_signal(turn_sem.at[n], inc=1, device_id=peers[bit], device_id_type=MESH)
        for n in range(3):
            pl.semaphore_wait(turn_sem.at[n], 1)
        reduce.start()

    def middle(first):
        @pl.when(pair > 0)
        def _():
            (reduce.mid1 if first else reduce.mid2)()

        @pl.when(pair > 1)
        def _():
            (gather.mid1 if first else gather.mid2)()

    seq = q_ref.shape[0]
    n_blk = seq // BLK
    half = lax.rem(pair, 2)

    def setup_block(i, carry):
        rows = aligned(i * LANES, LANES)
        cos_v, sin_v = cos_ref[rows, :], sin_ref[rows, :]
        for c in range(2):
            q_s[c, rows, :] = (lane_rotate(q_ref[rows, pl.ds(c * LANES, LANES)], cos_v, sin_v) * 0.125).astype(jnp.bfloat16)
        for vals, var, turned in ((lane_rotate(k_ref[rows, :], cos_v, sin_v), k_var, k_t), (v_ref[rows, :], v_var, v_t)):
            half_variants(vals.astype(jnp.bfloat16).astype(jnp.float32), half, var, turned, rows)
        return carry

    lax.fori_loop(0, seq // LANES, setup_block, 0, unroll=4)

    def grad_attn(n, carry):
        rows = aligned(n * TALL, TALL)
        block = dot_nt(gy_ref[rows, :], wo_ref[...]).astype(jnp.bfloat16)
        do_s[0, rows, :] = block[:, :LANES]
        do_s[1, rows, :] = block[:, LANES:]
        return carry

    lax.fori_loop(0, seq // TALL, grad_attn, 0, unroll=2)
    middle(True)
    dk_acc[...] = jnp.zeros_like(dk_acc)
    dv_acc[...] = jnp.zeros_like(dv_acc)
    low = low_half((BLK, LANES))

    def head_pair(hp, carry):
        for i in range(n_blk):
            rows = pl.ds(i * BLK, BLK)
            q_blk = q_s[hp, rows, :]
            do_blk = do_s[hp, rows, :]
            parts = [(pl.ds(i * BLK, BLK), True)]
            if i:
                parts.append((pl.ds(0, i * BLK), False))
            dv_sum, dk_sum = [0.0] * len(parts), [0.0] * len(parts)
            for par in range(2):
                sub_h = aligned(hp * LANES + par * HEAD, HEAD)
                q_mine = jnp.where(low != par, q_blk, jnp.zeros_like(q_blk))
                do_mine = jnp.where(low != par, do_blk, jnp.zeros_like(do_blk))
                scores, top = [], None
                for keys, is_diag in parts:
                    part = dot_nt(k_var[par, keys, :], q_blk)
                    if is_diag:
                        part = causal_diag(part)
                    scores.append(part)
                    part_top = over_keys(jnp.max, part)
                    top = part_top if top is None else jnp.maximum(top, part_top)
                exps = [jnp.exp(part - top) for part in scores]
                inv = 1.0 / sum(over_keys(jnp.sum, part) for part in exps)
                probs, grads, row_dot, attn = [], [], 0.0, 0.0
                for n, (keys, _) in enumerate(parts):
                    prob = exps[n] * inv
                    prob_b = prob.astype(jnp.bfloat16)
                    grad_p = dot_nt(v_var[par, keys, :], do_blk)
                    row_dot = row_dot + over_keys(jnp.sum, prob * grad_p)
                    attn = attn + dot_nn(v_t[:, keys], prob_b)
                    dv_sum[n] = dv_sum[n] + dot_nn(prob_b, do_mine)
                    probs.append(prob)
                    grads.append(grad_p)
                ot_ref[sub_h, rows] = attn.astype(jnp.bfloat16)
                acc = 0.0
                for n, (keys, _) in enumerate(parts):
                    grad_s = (probs[n] * (grads[n] - row_dot)).astype(jnp.bfloat16)
                    dk_sum[n] = dk_sum[n] + dot_nn(grad_s, q_mine)
                    acc = acc + dot_nn(k_t[:, keys], grad_s)
                dq_t[sub_h, rows] = acc
            for n, (keys, _) in enumerate(parts):
                dv_acc[keys, :] += dv_sum[n]
                dk_acc[keys, :] += dk_sum[n]
        return carry

    lax.fori_loop(0, 2, head_pair, 0)

    def finish_block(i, carry):
        rows = aligned(i * LANES, LANES)
        cos_v, sin_v = cos_ref[rows, :], -sin_ref[rows, :]
        for c in range(2):
            cols = pl.ds(c * LANES, LANES)
            o_ref[rows, cols] = jnp.transpose(ot_ref[cols, rows])
            grad_q = jnp.transpose(dq_t[cols, rows]) * 0.125
            out_ref[rows, cols] = lane_rotate(grad_q, cos_v, sin_v).astype(jnp.bfloat16)
        grad_k, grad_v = (ref[rows, :] + pltpu.roll(ref[rows, :], HEAD, 1) for ref in (dk_acc, dv_acc))
        out_ref[rows, KV_COLS] = jnp.where(low_half(grad_k.shape), lane_rotate(grad_k, cos_v, sin_v), grad_v).astype(jnp.bfloat16)
        return carry

    lax.fori_loop(0, seq // LANES, finish_block, 0, unroll=4)
    mine = coord[1]
    rows_q, rows_d = own[0].shape[0], own[1].shape[0]

    def weight_q(n, carry):
        rows = aligned(n * TALL, TALL)
        for side, ref in ((1 - mine, sent[0]), (mine, own[0])):
            ref[rows, :] = dot_nn(normed_ref[aligned(side * rows_q + n * TALL, TALL), :], out_ref[...]).astype(ref.dtype)
        return carry

    def weight_d(n, carry):
        cols = aligned(n * BLK, BLK)
        both = dot_nn(ot_ref[...], gy_ref[:, cols])
        top, bottom = both[:rows_d], both[rows_d:]
        own[1][:, cols] = jnp.where(mine == 0, top, bottom)
        sent[1][:, cols] = jnp.where(mine == 0, bottom, top).astype(jnp.bfloat16)
        return carry

    middle(False)
    lax.fori_loop(0, rows_q // TALL, weight_q, 0, unroll=2)
    lax.fori_loop(0, gy_ref.shape[1] // BLK, weight_d, 0, unroll=4)

    @pl.when(pair > 0)
    def _():
        reduce.end()

    @pl.when(pair > 1)
    def _():
        gather.end()

    @pl.when(jnp.logical_and(pair > 0, pair < pl.num_programs(0) - 1))
    def _():
        upcoming.start()

    @pl.when(pair == pl.num_programs(0) - 1)
    def _():
        outs = [sent_q_out, sent_d_out, own_q_out, own_d_out, total_q_out, total_d_out]
        copies = [pltpu.make_async_copy(src, dst, out_sem.at[n]) for n, (src, dst) in enumerate(zip(sent + own + total, outs))]
        for copy in copies:
            copy.start()
        for copy in copies:
            copy.wait()


def total_shapes(own):
    return [jax.ShapeDtypeStruct((2, o.shape[0] // 8, o.shape[1]), jnp.bfloat16) for o in own]


def piece_shapes(total):
    return [jax.ShapeDtypeStruct((16,) + t.shape[1:], jnp.bfloat16) for t in total]


def attention(qkv, w_o, cos_t, sin_t, normed_t, grad_y):
    seq, d_model = grad_y.shape
    n_steps = qkv.shape[1] // GROUP_W
    const = lambda shape: pl.BlockSpec(shape, lambda p: (0,) * len(shape), pipeline_mode=pl.Buffered(1))
    col = lambda width: pl.BlockSpec((seq, width), lambda p: (0, p))
    of_pair = lambda at: pl.BlockSpec((seq, LANES), lambda p: (0, p // 2 * (PAIR_W // LANES) + at))
    anywhere = pl.BlockSpec(memory_space=pl.ANY)
    shape = jax.ShapeDtypeStruct
    slab = pltpu.VMEM((2, seq, LANES), jnp.bfloat16)
    turned = pltpu.VMEM((HEAD, seq), jnp.bfloat16)
    acc = pltpu.VMEM((seq, LANES), jnp.float32)
    partial = [(d_model // 2, GROUP_W), (Q_COLS // 2, d_model)]
    own = [shape(p, jnp.float32) for p in partial]
    sent = [shape(p, jnp.bfloat16) for p in partial]
    totals = total_shapes(own)
    pieces = [shape((n_steps - 2,) + p.shape, p.dtype) for p in piece_shapes(totals)]
    kept = [pltpu.VMEM(p.shape, p.dtype) for p in sent + own + totals]
    out = pl.pallas_call(
        attn_kernel,
        grid=(n_steps,),
        in_specs=[pl.BlockSpec((seq, Q_COLS), lambda p: (0, p // 2 * (PAIR_W // Q_COLS) + p % 2)), of_pair(4), of_pair(5), pl.BlockSpec((Q_COLS, d_model), lambda p: (p, 0)), const((seq, LANES)), const((seq, LANES)), const((d_model, seq)), const((seq, d_model))],
        out_specs=[col(Q_COLS), col(GROUP_W)] + [anywhere] * 8,
        out_shape=[shape((seq, Q_COLS * n_steps), jnp.bfloat16), shape((seq, GROUP_W * n_steps), jnp.bfloat16)] + sent + own + totals + pieces,
        scratch_shapes=[slab, slab, slab, slab, turned, turned, pltpu.VMEM((Q_COLS, seq), jnp.bfloat16), pltpu.VMEM((Q_COLS, seq), jnp.float32), acc, acc]
        + kept + Reduce.scratch_shapes(partial) + Gather.scratch_shapes(2)
        + [pltpu.SemaphoreType.REGULAR((3,)), pltpu.SemaphoreType.DMA((6,))],
        compiler_params=pltpu.CompilerParams(vmem_limit_bytes=VMEM_LIMIT, collective_id=0, has_side_effects=True),
        cost_estimate=pl.CostEstimate(flops=COST_FLOPS, bytes_accessed=COST_BYTES, transcendentals=COST_BYTES),
        name="attn",
    )(qkv, qkv, qkv, w_o, cos_t, sin_t, normed_t, grad_y)
    return out[0], out[1], (list(out[2:4]), list(out[4:6])), list(out[6:8]), out[8:10]


def finish_kernel(o_ref, x_ref, grads_ref, gy_ref, gain_ref, wo_ref, w_hbm, sent_q, sent_d, own_q, own_d, old_q, old_d,
                  y_out, gh_out, old_pieces_q, old_pieces_d, pieces_q, pieces_d, norm_out, *scratch):
    scratch = list(scratch)
    take = lambda n: [scratch.pop(0) for _ in range(n)]
    y_s, gh_s, w_s, dh_s, norm_ref, norm_row, norm_all = take(7)
    total = take(2)
    step = pl.program_id(0)
    me = lax.axis_index('sp')
    coord, peers = axis_bits()
    reduce = Reduce(coord, peers, [sent_q, sent_d], [own_q, own_d], total, take(16))
    gather = Gather(peers, [old_q, old_d], [old_pieces_q, old_pieces_d], take(3))
    last = Gather(peers, total, [pieces_q, pieces_d], take(3))
    w_sem, y_send, y_recv, gh_send, gh_recv, norm_send, norm_recv = take(7)
    n_devs = y_out.shape[0]
    tok = y_out.shape[1]
    half_steps = pl.num_programs(0) // 2
    per_step = n_devs // half_steps
    weights = load_weights(w_hbm, w_s, w_sem, (0, GROUP_W, Q_COLS, PAIR_W - LANES))

    def share(values, out, send_sem, recv_sem, dest, act):
        @pl.when(dest == me)
        def _():
            act(pltpu.make_async_copy(values.at[dest], out.at[dest], send_sem.at[dest]), True)

        @pl.when(dest != me)
        def _():
            act(pltpu.make_async_remote_copy(src_ref=values.at[dest], dst_ref=out.at[me], send_sem=send_sem.at[dest], recv_sem=recv_sem.at[me],
                                             device_id={'sp': dest}, device_id_type=MESH), False)

    def send(values, out, send_sem, recv_sem, dests):
        for dest in dests:
            share(values, out, send_sem, recv_sem, dest, lambda copy, local: copy.start())

    def finish(values, out, send_sem, recv_sem):
        for peer in range(n_devs):
            @pl.when(peer == me)
            def _():
                pltpu.make_async_copy(values.at[peer], out.at[peer], send_sem.at[peer]).wait()

            @pl.when(peer != me)
            def _():
                pltpu.make_async_remote_copy(src_ref=values.at[peer], dst_ref=out.at[peer], send_sem=send_sem.at[peer], recv_sem=recv_sem.at[peer],
                                             device_id={'sp': peer}, device_id_type=MESH).wait()

    def share_norm(act):
        for k in range(1, n_devs):
            peer = lax.rem(me + k, n_devs)
            copy = pltpu.make_async_remote_copy(src_ref=norm_row, dst_ref=norm_all.at[me], send_sem=norm_send.at[k], recv_sem=norm_recv.at[k],
                                                device_id={'sp': peer}, device_id_type=MESH)
            act(copy)

    @pl.when(step == 0)
    def _():
        greet_all(me, n_devs)
        reduce.start()
        gather.start()
        for copy in weights:
            copy.start()
        norm_ref[...] = jnp.zeros_like(norm_ref)

    @pl.when(step == 1)
    def _():
        reduce.mid1()
        gather.mid1()

    @pl.when(jnp.logical_and(step >= 1, step <= half_steps))
    def _():
        send(y_s, y_out, y_send, y_recv, [(step - 1) * per_step + k for k in range(per_step)])

    d_model = wo_ref.shape[1]

    @pl.when(step < half_steps)
    def _():
        def cols_of_y(n, carry):
            cols = aligned(n * 512, 512)
            block = (x_ref[:, cols].astype(jnp.float32) + dot_nn(o_ref[...], wo_ref[:, cols])).astype(jnp.bfloat16)
            for k in range(per_step):
                y_s[step * per_step + k, :, cols] = block[k * tok:(k + 1) * tok, :]
            return carry
        lax.fori_loop(0, d_model // 512, cols_of_y, 0)

    @pl.when(step == half_steps)
    def _():
        for copy in weights:
            copy.wait()

        def pair_up(n, carry):
            rows = aligned(n * LANES, LANES)
            for pair in range(w_s.shape[1] // PAIR_W):
                spots = [pl.ds(pair * PAIR_W + at, LANES) for at in (Q_COLS, PAIR_W - LANES)]
                for spot, cols in zip(spots, cross(*[w_s[rows, spot].astype(jnp.float32) for spot in spots])):
                    w_s[rows, spot] = cols.astype(jnp.bfloat16)
            return carry

        lax.fori_loop(0, d_model // LANES, pair_up, 0)

    @pl.when(step >= half_steps)
    def _():
        def cols_of_dh(n, carry):
            rows = aligned(n * 512, 512)
            dh_s[:, rows] = dot_nt(grads_ref[...], w_s[rows, :])
            return carry
        lax.fori_loop(0, d_model // 512, cols_of_dh, 0)
        gain = gain_ref[...]

        def norm_rows(n, carry):
            rows = aligned(n * 16, 16)
            x_f = x_ref[rows, :].astype(jnp.float32)
            inv_rms = lax.rsqrt(jnp.mean(x_f * x_f, axis=-1, keepdims=True) + NORM_EPS)
            unit = x_f * inv_rms
            grad_normed = dh_s[rows, :]
            grad_unit = grad_normed * gain
            mean_dot = jnp.mean(grad_unit * unit, axis=-1, keepdims=True)
            grad_x = gy_ref[rows, :].astype(jnp.float32) + inv_rms * (grad_unit - unit * mean_dot)
            place = (step - half_steps) * per_step + n // (tok // 16)
            gh_s[place, aligned(lax.rem(n, tok // 16) * 16, 16), :] = grad_x.astype(jnp.bfloat16)
            weighted = grad_normed * unit
            norm_ref[...] += weighted[:8, :] + weighted[8:, :]
            return carry
        lax.fori_loop(0, per_step * tok // 16, norm_rows, 0)

    @pl.when(step == pl.num_programs(0) - 1)
    def _():
        gh = (gh_s, gh_out, gh_send, gh_recv)
        norm_row[...] = over_keys(jnp.sum, norm_ref[...])
        reduce.mid2()
        gather.mid2()
        share_norm(lambda copy: copy.start())
        send(*gh, range(n_devs // 2))
        reduce.end()
        last.start()
        send(*gh, range(n_devs // 2, n_devs))
        gather.end()
        last.mid1()
        last.mid2()
        share_norm(lambda copy: copy.wait())
        norm_all[me] = norm_row[...]
        norm_out[...] = sum(norm_all[peer] for peer in range(n_devs))
        finish(y_s, y_out, y_send, y_recv)
        last.end()
        finish(*gh)


def finish(attn, x, grads, grad_y, gain, w_o, w_qkv, reduce, old_total, n_devs):
    seq, d_model = x.shape
    sent, own = reduce
    steps = 8
    rows = 2 * seq // steps
    tok = seq // n_devs
    const = lambda shape: pl.BlockSpec(shape, lambda s: (0,) * len(shape), pipeline_mode=pl.Buffered(1))
    early = lambda width: pl.BlockSpec((rows, width), lambda s: (jnp.minimum(s, steps // 2 - 1), 0))
    late = lambda width: pl.BlockSpec((rows, width), lambda s: (jnp.maximum(s - steps // 2, 0), 0))
    anywhere = pl.BlockSpec(memory_space=pl.ANY)
    shape = jax.ShapeDtypeStruct
    totals = total_shapes(own)
    tokens = shape((n_devs, tok, d_model), jnp.bfloat16)
    dma = lambda: pltpu.SemaphoreType.DMA((n_devs,))
    out = pl.pallas_call(
        finish_kernel,
        grid=(steps,),
        in_specs=[early(q_w) for q_w in (attn.shape[1],)] + [pl.BlockSpec((rows, d_model), lambda s: (lax.rem(s, steps // 2), 0)), late(grads.shape[1]), late(d_model),
                  const((1, d_model)), const(w_o.shape), anywhere, anywhere, anywhere]
        + [const(o.shape) for o in own] + [const(t.shape) for t in totals],
        out_specs=[anywhere] * 6 + [pl.BlockSpec((1, d_model), lambda s: (0, 0))],
        out_shape=[tokens, tokens] + piece_shapes(totals) + piece_shapes(totals) + [shape((1, d_model), jnp.float32)],
        scratch_shapes=[pltpu.VMEM(tokens.shape, jnp.bfloat16), pltpu.VMEM(tokens.shape, jnp.bfloat16),
                        pltpu.VMEM(w_qkv.shape, jnp.bfloat16), pltpu.VMEM((rows, d_model), jnp.float32),
                        pltpu.VMEM((8, d_model), jnp.float32), pltpu.VMEM((1, d_model), jnp.float32),
                        pltpu.VMEM((n_devs, 1, d_model), jnp.float32)]
        + [pltpu.VMEM(t.shape, t.dtype) for t in totals]
        + Reduce.scratch_shapes([o.shape for o in own]) + Gather.scratch_shapes(2) + Gather.scratch_shapes(2)
        + [pltpu.SemaphoreType.DMA((4 * w_qkv.shape[1] // PAIR_W,))] + [dma()] * 6,
        compiler_params=pltpu.CompilerParams(vmem_limit_bytes=VMEM_LIMIT, collective_id=1, has_side_effects=True),
        cost_estimate=pl.CostEstimate(flops=COST_FLOPS, bytes_accessed=COST_BYTES, transcendentals=COST_BYTES),
        name="finish",
    )(attn, x, grads, grad_y, gain, w_o, w_qkv, *sent, *own, *old_total)
    return out[0], out[1], out[2:4], out[4:6], out[6]


def place_kernel(n, slots, *refs):
    pieces_q, pieces_d, tokens = refs[:n], refs[n:2 * n], refs[2 * n:2 * n + 2]
    q_out, d_out, *tokens_out = refs[2 * n + 2:]
    for src, dst in zip(tokens, tokens_out):
        dst[...] = src[...]
    for c in range(n):
        d_out[c] = pieces_d[c][0, 0].astype(jnp.float32)
        q_out[:, pl.ds(c * Q_COLS, Q_COLS)] = pieces_q[c][0, 0, :, :Q_COLS].astype(jnp.float32)
    for pair in range(n // 2):
        grads = cross(*[ref[0, 0, :, Q_COLS:].astype(jnp.float32) for ref in pieces_q[2 * pair:2 * pair + 2]])
        for at, grad in zip((n * Q_COLS, q_out.shape[1] - n * HEAD), grads):
            q_out[:, pl.ds(at + pair * LANES, LANES)] = grad


def place(slots, parts_q, parts_d, tokens):
    specs, args, sizes = [], [], []
    for parts in (parts_q, parts_d):
        chunks = [(part, c) for part in parts for c in range(part.shape[0])]
        rows, width = parts[0].shape[2:]
        specs += [pl.BlockSpec((1, 1, rows, width), lambda s, slots, c=c: (c, s, 0, 0)) for _, c in chunks]
        args += [part for part, _ in chunks]
        sizes.append((len(chunks), rows, width))
    (n_pairs, rows_q, width_q), (_, rows_d, width_d) = sizes
    flat = [t.reshape(16, -1, t.shape[-1]) for t in tokens]
    through = pl.BlockSpec((1,) + flat[0].shape[1:], lambda s, slots: (s, 0, 0))
    shape = jax.ShapeDtypeStruct
    grad_q, grad_d, *out = pl.pallas_call(
        functools.partial(place_kernel, n_pairs),
        grid_spec=pltpu.PrefetchScalarGridSpec(
            num_scalar_prefetch=1, grid=(16,), in_specs=specs + [through] * 2,
            out_specs=[pl.BlockSpec((rows_q, n_pairs * width_q), lambda s, slots: (slots[s], 0)),
                       pl.BlockSpec((n_pairs, rows_d, width_d), lambda s, slots: (0, slots[s], 0)), through, through]),
        out_shape=[shape((16 * rows_q, n_pairs * width_q), jnp.float32), shape((n_pairs, 16 * rows_d, width_d), jnp.float32)]
        + [shape(t.shape, t.dtype) for t in flat],
        compiler_params=pltpu.CompilerParams(vmem_limit_bytes=VMEM_LIMIT),
        cost_estimate=pl.CostEstimate(flops=COST_FLOPS, bytes_accessed=COST_BYTES, transcendentals=COST_BYTES),
        name="place",
    )(slots, *args, *flat)
    return grad_q, grad_d, [o.reshape(t.shape) for o, t in zip(out, tokens)]


def row_slots():
    me = lax.axis_index('sp')
    core, x, y = me & 1, (me >> 1) & 1, me >> 2
    order = []
    for c in (core, 1 - core):
        for half, (a, b) in enumerate(((x, y), (y, x))):
            for a_i in (a, 1 - a):
                for b_i in (b, 1 - b):
                    order.append(c * 8 + half * 4 + a_i * 2 + b_i)
    return jnp.stack(order).astype(jnp.int32)


def solution(mesh):
    n_devs = mesh.shape['sp']

    def device_step(hidden, norm_w, w_qkv, w_out, long_factor, grad_out):
        d_model = hidden.shape[-1]
        gain = norm_w.astype(jnp.float32)[None]
        x, grad_y, qkv, normed_t, cos_t, sin_t = enter(hidden, grad_out, gain, inverse_frequencies(long_factor), w_qkv)
        x, grad_y = x.reshape(-1, d_model), grad_y.reshape(-1, d_model)
        w_o = w_out.reshape(-1, d_model)
        attn, grads, partial, total, pieces = attention(qkv, w_o, cos_t, sin_t, normed_t, grad_y)
        block_out, grad_hidden, before_last, last, grad_norm_w = finish(attn, x, grads, grad_y, gain, w_o, w_qkv, partial, total, n_devs)
        parts = [[first, second[None], third[None]] for first, second, third in zip(pieces, before_last, last)]
        grad_w_qkv, grad_w_out, (block_out, grad_hidden) = place(row_slots(), *parts, (block_out, grad_hidden))
        return block_out, grad_hidden, grad_w_qkv, grad_w_out.reshape(w_out.shape), grad_norm_w.reshape(-1)

    tok_spec = P('dp', 'sp', None)
    return jax.shard_map(device_step, mesh=mesh,
                         in_specs=(tok_spec, P(), P(), P(), P(), tok_spec),
                         out_specs=(tok_spec, tok_spec, P('dp', None), P('dp', None, None), P('dp')),
                         check_vma=False)
```

```python
import functools
import math
import jax
import jax.numpy as jnp
from jax import lax
from jax.experimental import pallas as pl
from jax.experimental.pallas import tpu as pltpu
from jax.sharding import PartitionSpec as P

NORM_EPS = 1e-5
ROPE_BASE = 10000.0
ROPE_GAIN = math.sqrt(1.0 + math.log(32.0) / math.log(4096.0))
MASK_VALUE = -1e30
BLK = 256
TALL = 512
LANES = 128
HEAD = LANES // 2
Q_COLS = 2 * LANES
GROUP_W = Q_COLS + LANES
PAIR_W = 2 * GROUP_W
KV_COLS = pl.ds(Q_COLS, LANES)
MESH = pl.DeviceIdType.MESH
VMEM_LIMIT = 67_000_000
COST_BYTES = 2**26
COST_FLOPS = 10**11


def inverse_frequencies(long_factor):
    half_rot = long_factor.shape[0]
    exponent = jnp.arange(half_rot, dtype=jnp.float32) / half_rot
    inv_freq = 1.0 / (long_factor * jnp.power(ROPE_BASE, exponent))
    return jnp.tile(inv_freq, LANES // half_rot)[None]


def first_quarter(shape):
    return lax.broadcasted_iota(jnp.int32, shape, 1) % HEAD < HEAD // 2


def lane_rotate(vals, cos_v, sin_v):
    first = first_quarter(vals.shape)
    partner = jnp.where(first, pltpu.roll(vals, LANES - 32, 1), pltpu.roll(vals, 32, 1))
    return vals * cos_v + partner * sin_v


def low_half(shape):
    return lax.broadcasted_iota(jnp.int32, shape, 1) < HEAD


def cross(a, b):
    low = low_half(a.shape)
    return jnp.where(low, a, pltpu.roll(b, HEAD, 1)), jnp.where(low, pltpu.roll(a, HEAD, 1), b)


def half_variants(vals, half, out_ref, turned_ref, rows):
    low = low_half(vals.shape)
    swapped = pltpu.roll(vals, HEAD, 1)
    first, second = jnp.where(half == 0, vals, swapped), jnp.where(half == 0, swapped, vals)
    out_ref[0, rows, :] = jnp.where(low, first, 0.0).astype(jnp.bfloat16)
    out_ref[1, rows, :] = jnp.where(low, 0.0, second).astype(jnp.bfloat16)
    turned_ref[:, rows] = jnp.transpose(first)[:HEAD].astype(jnp.bfloat16)


def over_keys(reduce, vals):
    return reduce(vals, axis=0, keepdims=True)


def aligned(start, size):
    return pl.ds(pl.multiple_of(start, size), size)


def dot_nt(a, b):
    return lax.dot_general(a, b, (((1,), (1,)), ((), ())), preferred_element_type=jnp.float32)


def dot_nn(a, b):
    return lax.dot_general(a, b, (((1,), (0,)), ((), ())), preferred_element_type=jnp.float32)


def causal_diag(scores):
    keys = lax.broadcasted_iota(jnp.int32, scores.shape, 0)
    rows = lax.broadcasted_iota(jnp.int32, scores.shape, 1)
    return jnp.where(keys <= rows, scores, MASK_VALUE)


def load_weights(w_hbm, w_s, sem, places):
    width = w_hbm.shape[1]
    n_pairs = width // PAIR_W
    copies = []
    for pair in range(n_pairs):
        q, k, v = pair * 2 * Q_COLS, n_pairs * 2 * Q_COLS + pair * LANES, width - (n_pairs - pair) * LANES
        for src, cols, dst in zip((q, q + Q_COLS, k, v), (Q_COLS, Q_COLS, LANES, LANES), places):
            copies.append(pltpu.make_async_copy(w_hbm.at[:, pl.ds(src, cols)], w_s.at[:, pl.ds(pair * PAIR_W + dst, cols)], sem.at[len(copies)]))
    return copies


def greet_all(me, n_devs):
    barrier = pltpu.get_barrier_semaphore()
    for k in range(1, n_devs):
        pl.semaphore_signal(barrier, inc=1, device_id={'sp': lax.rem(me + k, n_devs)}, device_id_type=MESH)
    pl.semaphore_wait(barrier, n_devs - 1)


def enter_kernel(hidden, grad_out, gain_ref, freq_ref, w_hbm, x_out, gy_out, qkv_out, turned_out, cos_out, sin_out, x_s, own_s, w_s, h_s, turned_s, stage,
                 x_send, x_recv, gy_send, gy_recv, w_sem, out_sem, stage_sem):
    n_devs, tok, d_model = hidden.shape
    me = lax.axis_index('sp')

    def to_peer(src, dst, send_sem, recv_sem, k):
        peer = lax.rem(me + k, n_devs)
        return pltpu.make_async_remote_copy(src_ref=src.at[peer], dst_ref=dst.at[me], send_sem=send_sem.at[k], recv_sem=recv_sem.at[k],
                                            device_id={'sp': peer}, device_id_type=MESH)

    weights = load_weights(w_hbm, w_s, w_sem, (0, Q_COLS, 2 * Q_COLS, PAIR_W - LANES))
    own_x = pltpu.make_async_copy(hidden.at[me], x_s.at[me], x_send.at[0])
    own_in = pltpu.make_async_copy(grad_out.at[me], own_s, gy_send.at[0])
    own_out = pltpu.make_async_copy(own_s, gy_out.at[me], gy_recv.at[0])
    greet_all(me, n_devs)
    peers = range(1, n_devs)
    xs = [to_peer(hidden, x_s, x_send, x_recv, k) for k in peers]
    gys = [to_peer(grad_out, gy_out, gy_send, gy_recv, k) for k in peers]
    for copy in xs + gys + [own_x, own_in] + weights:
        copy.start()
    gain = gain_ref[...]

    def norm_block(block):
        def norm_rows(n, carry):
            rows = aligned(n * 16, 16)
            x_f = x_s[block, rows, :].astype(jnp.float32)
            inv_rms = lax.rsqrt(jnp.mean(x_f * x_f, axis=-1, keepdims=True) + NORM_EPS)
            h_s[block, rows, :] = (x_f * inv_rms * gain).astype(jnp.bfloat16)
            return carry
        lax.fori_loop(0, tok // 16, norm_rows, 0)

    own_x.wait()
    norm_block(me)
    for k, copy in zip(peers, xs):
        copy.wait()
        norm_block(lax.rem(me + n_devs - k, n_devs))
    own_in.wait()
    own_out.start()
    for copy in weights:
        copy.wait()
    keep_x = pltpu.make_async_copy(x_s, x_out, out_sem.at[0])
    keep_x.start()

    def keep_qkv(pair):
        return pltpu.make_async_copy(stage.at[pair % 2], qkv_out.at[:, pl.ds(pair * PAIR_W, PAIR_W)], stage_sem.at[pair % 2])

    half = n_devs // 2
    n_pairs = w_hbm.shape[1] // PAIR_W
    for pair in range(n_pairs):
        if pair > 1:
            keep_qkv(pair - 2).wait()

        def columns(n, carry):
            for m in range(2):
                left = h_s[pl.ds(m * half, half)].reshape(half * tok, d_model)
                stage[pair % 2, pl.ds(m * half * tok, half * tok), aligned(n * BLK, BLK)] = dot_nn(left, w_s[:, aligned(pair * PAIR_W + n * BLK, BLK)])
            return carry

        lax.fori_loop(0, PAIR_W // BLK, columns, 0)
        keep_qkv(pair).start()

    def turn(n, carry):
        cols = aligned(n * LANES, LANES)
        for block in range(n_devs):
            turned_s[cols, pl.ds(block * tok, tok)] = jnp.transpose(h_s[block, :, cols])
        return carry

    lax.fori_loop(0, d_model // LANES, turn, 0)

    def tables(n, carry):
        rows = aligned(n * LANES, LANES)
        angles = (lax.broadcasted_iota(jnp.int32, (LANES, LANES), 0) + n * LANES).astype(jnp.float32) * freq_ref[...]
        cos_out[rows, :] = jnp.cos(angles) * ROPE_GAIN
        sin_v = jnp.sin(angles) * ROPE_GAIN
        sin_out[rows, :] = jnp.where(first_quarter(angles.shape), -sin_v, sin_v)
        return carry

    lax.fori_loop(0, cos_out.shape[0] // LANES, tables, 0)
    keep_turned = pltpu.make_async_copy(turned_s, turned_out, out_sem.at[1])
    keep_turned.start()
    for copy in gys:
        copy.wait()
    for pair in range(n_pairs - 2, n_pairs):
        keep_qkv(pair).wait()
    keep_turned.wait()
    keep_x.wait()
    own_out.wait()


def enter(hidden, grad_out, gain, freq, w_qkv):
    n_devs, tok, d_model = hidden.shape
    seq, width = n_devs * tok, w_qkv.shape[1]
    anywhere, vmem, dma = pl.BlockSpec(memory_space=pl.ANY), pltpu.VMEM, pltpu.SemaphoreType.DMA
    shape, bf16 = jax.ShapeDtypeStruct, jnp.bfloat16
    local = pl.BlockSpec(memory_space=vmem)
    return pl.pallas_call(
        enter_kernel,
        in_specs=[anywhere, anywhere, local, local, anywhere],
        out_specs=[anywhere] * 4 + [local] * 2,
        out_shape=[shape(hidden.shape, bf16), shape(hidden.shape, bf16), shape((seq, width), jnp.float32), shape((d_model, seq), bf16)]
        + [shape((seq, LANES), jnp.float32)] * 2,
        scratch_shapes=[vmem(hidden.shape, bf16), vmem((tok, d_model), bf16), vmem(w_qkv.shape, bf16), vmem(hidden.shape, bf16),
                        vmem((d_model, seq), bf16), vmem((2, seq, PAIR_W), jnp.float32)]
        + [dma((n_devs,))] * 4 + [dma((4 * width // PAIR_W,)), dma((2,)), dma((2,))],
        compiler_params=pltpu.CompilerParams(vmem_limit_bytes=VMEM_LIMIT, collective_id=2, has_side_effects=True),
        cost_estimate=pl.CostEstimate(flops=COST_FLOPS, bytes_accessed=COST_BYTES, transcendentals=COST_BYTES),
        name="enter",
    )(hidden, grad_out, gain, freq, w_qkv)


def axis_bits():
    me = lax.axis_index('sp')
    coord = {1: lax.rem(me, 2), 2: lax.rem(lax.div(me, 2), 2), 4: lax.div(me, 4)}
    return coord, {bit: {'sp': me + bit * (1 - 2 * coord[bit])} for bit in (1, 2, 4)}


def entry_barrier(peers):
    barrier = pltpu.get_barrier_semaphore()
    for bit in (1, 2, 4):
        pl.semaphore_signal(barrier, inc=1, device_id=peers[bit], device_id_type=MESH)
    pl.semaphore_wait(barrier, 3)


ORDER_OF_HALF = ((2, 4), (4, 2))


def add_rows(dst_ref, a_ref, a_row, b_ref, b_row):
    def body(i, carry):
        step = pl.multiple_of(i * 16, 16)
        total = a_ref[aligned(a_row + step, 16), :] + b_ref[aligned(b_row + step, 16), :].astype(jnp.float32)
        dst_ref[pl.ds(step, 16), :] = total.astype(dst_ref.dtype)
        return carry
    lax.fori_loop(0, dst_ref.shape[0] // 16, body, 0)


class Reduce:
    def __init__(self, coord, peers, sent, own, total, scratch):
        self.coord, self.peers, self.sent, self.own, self.total = coord, peers, sent, own, total
        n = len(sent)
        self.recv_c, self.sum0, self.snd0, self.recv0, self.sum1, self.snd1, self.recv1 = (scratch[k * n:(k + 1) * n] for k in range(7))
        self.send_sem, self.recv_sem = scratch[7 * n:]
        self.n = n

    def copy(self, src, dst, sem, bit):
        return pltpu.make_async_remote_copy(src_ref=src, dst_ref=dst, send_sem=self.send_sem.at[sem], recv_sem=self.recv_sem.at[sem],
                                            device_id=self.peers[bit], device_id_type=MESH)

    def stage_c(self):
        return [self.copy(self.sent[t], self.recv_c[t], t, 1) for t in range(self.n)]

    def stage_s(self, k):
        snd, recv = (self.snd0, self.recv0) if k == 0 else (self.snd1, self.recv1)
        return [self.copy(snd[t].at[h], recv[t].at[h], self.n + 2 * self.n * k + 2 * t + h, ORDER_OF_HALF[h][k])
                for t in range(self.n) for h in range(2)]

    def start(self):
        for copy in self.stage_c():
            copy.start()

    def mid1(self):
        for copy in self.stage_c():
            copy.wait()
        for t in range(self.n):
            half = self.own[t].shape[0] // 2
            for h in range(2):
                c = self.coord[ORDER_OF_HALF[h][0]]
                row = h * half + (1 - c) * (half // 2)
                add_rows(self.snd0[t].at[h], self.own[t], row, self.recv_c[t], row)
        for copy in self.stage_s(0):
            copy.start()
        for t in range(self.n):
            half = self.own[t].shape[0] // 2
            for h in range(2):
                row = h * half + self.coord[ORDER_OF_HALF[h][0]] * (half // 2)
                add_rows(self.sum0[t].at[h], self.own[t], row, self.recv_c[t], row)

    def mid2(self):
        for copy in self.stage_s(0):
            copy.wait()
        for t in range(self.n):
            quarter = self.own[t].shape[0] // 4
            for h in range(2):
                row = (1 - self.coord[ORDER_OF_HALF[h][1]]) * (quarter // 2)
                add_rows(self.snd1[t].at[h], self.sum0[t].at[h], row, self.recv0[t].at[h], row)
        for copy in self.stage_s(1):
            copy.start()
        for t in range(self.n):
            quarter = self.own[t].shape[0] // 4
            for h in range(2):
                row = self.coord[ORDER_OF_HALF[h][1]] * (quarter // 2)
                add_rows(self.sum1[t].at[h], self.sum0[t].at[h], row, self.recv0[t].at[h], row)

    def end(self):
        for copy in self.stage_s(1):
            copy.wait()
        for t in range(self.n):
            for h in range(2):
                add_rows(self.total[t].at[h], self.sum1[t].at[h], 0, self.recv1[t].at[h], 0)

    @staticmethod
    def scratch_shapes(shapes):
        vmem = lambda dtype, div: [pltpu.VMEM((2, r // div, c) if div else (r, c), dtype) for r, c in shapes]
        n = len(shapes)
        return (vmem(jnp.bfloat16, 0) + vmem(jnp.float32, 4) + vmem(jnp.bfloat16, 4) + vmem(jnp.bfloat16, 4)
                + vmem(jnp.float32, 8) + vmem(jnp.bfloat16, 8) + vmem(jnp.bfloat16, 8)
                + [pltpu.SemaphoreType.DMA((5 * n,)), pltpu.SemaphoreType.DMA((5 * n,))])


class Gather:
    def __init__(self, peers, total, pieces, scratch):
        self.peers, self.total, self.pieces = peers, total, pieces
        self.send_sem, self.recv_sem, self.local_sem = scratch
        self.n = len(total)

    def copy(self, src, dst, sem, bit):
        return pltpu.make_async_remote_copy(src_ref=src, dst_ref=dst, send_sem=self.send_sem.at[sem], recv_sem=self.recv_sem.at[sem],
                                            device_id=self.peers[bit], device_id_type=MESH)

    def stage(self, k):
        copies = []
        for t in range(self.n):
            if k == 2:
                copies.append(self.copy(self.pieces[t].at[pl.ds(0, 8)], self.pieces[t].at[pl.ds(8, 8)], 4 * self.n + t, 1))
                continue
            for h in range(2):
                if k == 0:
                    src, dst = self.total[t].at[pl.ds(h, 1)], self.pieces[t].at[pl.ds(4 * h + 1, 1)]
                else:
                    src, dst = self.pieces[t].at[pl.ds(4 * h, 2)], self.pieces[t].at[pl.ds(4 * h + 2, 2)]
                copies.append(self.copy(src, dst, 2 * self.n * k + 2 * t + h, ORDER_OF_HALF[h][1 - k]))
        return copies

    def local(self):
        return [pltpu.make_async_copy(self.total[t].at[pl.ds(h, 1)], self.pieces[t].at[pl.ds(4 * h, 1)], self.local_sem.at[2 * t + h])
                for t in range(self.n) for h in range(2)]

    def start(self):
        for copy in self.stage(0) + self.local():
            copy.start()

    def mid1(self):
        for copy in self.stage(0) + self.local():
            copy.wait()
        for copy in self.stage(1):
            copy.start()

    def mid2(self):
        for copy in self.stage(1):
            copy.wait()
        for copy in self.stage(2):
            copy.start()

    def end(self):
        for copy in self.stage(2):
            copy.wait()

    @staticmethod
    def scratch_shapes(n):
        return [pltpu.SemaphoreType.DMA((5 * n,)), pltpu.SemaphoreType.DMA((5 * n,)), pltpu.SemaphoreType.DMA((2 * n,))]


def attn_kernel(q_ref, k_ref, v_ref, wo_ref, cos_ref, sin_ref, normed_ref, gy_ref,
                o_ref, out_ref, sent_q_out, sent_d_out, own_q_out, own_d_out, total_q_out, total_d_out, pieces_q, pieces_d, *scratch):
    scratch = list(scratch)
    take = lambda n: [scratch.pop(0) for _ in range(n)]
    q_s, do_s, k_var, v_var, k_t, v_t, ot_ref, dq_t, dk_acc, dv_acc = take(10)
    sent, own, total = take(2), take(2), take(2)
    pair = pl.program_id(0)
    coord, peers = axis_bits()
    reduce = Reduce(coord, peers, sent, own, total, take(16))
    chunk = jnp.maximum(pair - 2, 0)
    gather_sems = take(3)
    gather, upcoming = (Gather(peers, total, [ref.at[c] for ref in (pieces_q, pieces_d)], gather_sems)
                        for c in (chunk, lax.rem(pair + pieces_q.shape[0] - 1, pieces_q.shape[0])))
    turn_sem, out_sem = take(2)

    @pl.when(pair == 0)
    def _():
        entry_barrier(peers)

    @pl.when(pair > 0)
    def _():
        for n, bit in enumerate((1, 2, 4)):
            pl.semaphore_signal(turn_sem.at[n], inc=1, device_id=peers[bit], device_id_type=MESH)
        for n in range(3):
            pl.semaphore_wait(turn_sem.at[n], 1)
        reduce.start()

    def middle(first):
        @pl.when(pair > 0)
        def _():
            (reduce.mid1 if first else reduce.mid2)()

        @pl.when(pair > 1)
        def _():
            (gather.mid1 if first else gather.mid2)()

    seq = q_ref.shape[0]
    n_blk = seq // BLK
    half = lax.rem(pair, 2)

    def setup_block(i, carry):
        rows = aligned(i * LANES, LANES)
        cos_v, sin_v = cos_ref[rows, :], sin_ref[rows, :]
        for c in range(2):
            q_s[c, rows, :] = (lane_rotate(q_ref[rows, pl.ds(c * LANES, LANES)], cos_v, sin_v) * 0.125).astype(jnp.bfloat16)
        for vals, var, turned in ((lane_rotate(k_ref[rows, :], cos_v, sin_v), k_var, k_t), (v_ref[rows, :], v_var, v_t)):
            half_variants(vals.astype(jnp.bfloat16).astype(jnp.float32), half, var, turned, rows)
        return carry

    lax.fori_loop(0, seq // LANES, setup_block, 0, unroll=8)

    def grad_attn(n, carry):
        rows = aligned(n * TALL, TALL)
        block = dot_nt(gy_ref[rows, :], wo_ref[...]).astype(jnp.bfloat16)
        do_s[0, rows, :] = block[:, :LANES]
        do_s[1, rows, :] = block[:, LANES:]
        return carry

    lax.fori_loop(0, seq // TALL, grad_attn, 0, unroll=2)
    middle(True)
    dk_acc[...] = jnp.zeros_like(dk_acc)
    dv_acc[...] = jnp.zeros_like(dv_acc)
    low = low_half((BLK, LANES))

    def head_pair(hp, carry):
        for i in range(n_blk):
            rows = pl.ds(i * BLK, BLK)
            q_blk = q_s[hp, rows, :]
            do_blk = do_s[hp, rows, :]
            parts = [(pl.ds(i * BLK, BLK), True)]
            if i:
                parts.append((pl.ds(0, i * BLK), False))
            dv_sum, dk_sum = [0.0] * len(parts), [0.0] * len(parts)
            for par in range(2):
                sub_h = aligned(hp * LANES + par * HEAD, HEAD)
                q_mine = jnp.where(low != par, q_blk, jnp.zeros_like(q_blk))
                do_mine = jnp.where(low != par, do_blk, jnp.zeros_like(do_blk))
                scores, top = [], None
                for keys, is_diag in parts:
                    part = dot_nt(k_var[par, keys, :], q_blk)
                    if is_diag:
                        part = causal_diag(part)
                    scores.append(part)
                    part_top = over_keys(jnp.max, part)
                    top = part_top if top is None else jnp.maximum(top, part_top)
                exps = [jnp.exp(part - top) for part in scores]
                inv = 1.0 / sum(over_keys(jnp.sum, part) for part in exps)
                probs, grads, row_dot, attn = [], [], 0.0, 0.0
                for n, (keys, _) in enumerate(parts):
                    prob = exps[n] * inv
                    prob_b = prob.astype(jnp.bfloat16)
                    grad_p = dot_nt(v_var[par, keys, :], do_blk)
                    row_dot = row_dot + over_keys(jnp.sum, prob * grad_p)
                    attn = attn + dot_nn(v_t[:, keys], prob_b)
                    dv_sum[n] = dv_sum[n] + dot_nn(prob_b, do_mine)
                    probs.append(prob)
                    grads.append(grad_p)
                ot_ref[sub_h, rows] = attn.astype(jnp.bfloat16)
                acc = 0.0
                for n, (keys, _) in enumerate(parts):
                    grad_s = (probs[n] * (grads[n] - row_dot)).astype(jnp.bfloat16)
                    dk_sum[n] = dk_sum[n] + dot_nn(grad_s, q_mine)
                    acc = acc + dot_nn(k_t[:, keys], grad_s)
                dq_t[sub_h, rows] = acc
            for n, (keys, _) in enumerate(parts):
                dv_acc[keys, :] += dv_sum[n]
                dk_acc[keys, :] += dk_sum[n]
        return carry

    lax.fori_loop(0, 2, head_pair, 0, unroll=2)

    def finish_block(i, carry):
        rows = aligned(i * LANES, LANES)
        cos_v, sin_v = cos_ref[rows, :], -sin_ref[rows, :]
        for c in range(2):
            cols = pl.ds(c * LANES, LANES)
            o_ref[rows, cols] = jnp.transpose(ot_ref[cols, rows])
            grad_q = jnp.transpose(dq_t[cols, rows]) * 0.125
            out_ref[rows, cols] = lane_rotate(grad_q, cos_v, sin_v).astype(jnp.bfloat16)
        grad_k, grad_v = (ref[rows, :] + pltpu.roll(ref[rows, :], HEAD, 1) for ref in (dk_acc, dv_acc))
        out_ref[rows, KV_COLS] = jnp.where(low_half(grad_k.shape), lane_rotate(grad_k, cos_v, sin_v), grad_v).astype(jnp.bfloat16)
        return carry

    lax.fori_loop(0, seq // LANES, finish_block, 0, unroll=8)
    mine = coord[1]
    rows_q, rows_d = own[0].shape[0], own[1].shape[0]

    def weight_q(n, carry):
        rows = aligned(n * TALL, TALL)
        for side, ref in ((1 - mine, sent[0]), (mine, own[0])):
            ref[rows, :] = dot_nn(normed_ref[aligned(side * rows_q + n * TALL, TALL), :], out_ref[...]).astype(ref.dtype)
        return carry

    def weight_d(n, carry):
        cols = aligned(n * BLK, BLK)
        both = dot_nn(ot_ref[...], gy_ref[:, cols])
        top, bottom = both[:rows_d], both[rows_d:]
        own[1][:, cols] = jnp.where(mine == 0, top, bottom)
        sent[1][:, cols] = jnp.where(mine == 0, bottom, top).astype(jnp.bfloat16)
        return carry

    middle(False)
    lax.fori_loop(0, rows_q // TALL, weight_q, 0, unroll=2)
    lax.fori_loop(0, gy_ref.shape[1] // BLK, weight_d, 0, unroll=4)

    @pl.when(pair > 0)
    def _():
        reduce.end()

    @pl.when(pair > 1)
    def _():
        gather.end()

    @pl.when(jnp.logical_and(pair > 0, pair < pl.num_programs(0) - 1))
    def _():
        upcoming.start()

    @pl.when(pair == pl.num_programs(0) - 1)
    def _():
        outs = [sent_q_out, sent_d_out, own_q_out, own_d_out, total_q_out, total_d_out]
        copies = [pltpu.make_async_copy(src, dst, out_sem.at[n]) for n, (src, dst) in enumerate(zip(sent + own + total, outs))]
        for copy in copies:
            copy.start()
        for copy in copies:
            copy.wait()


def total_shapes(own):
    return [jax.ShapeDtypeStruct((2, o.shape[0] // 8, o.shape[1]), jnp.bfloat16) for o in own]


def piece_shapes(total):
    return [jax.ShapeDtypeStruct((16,) + t.shape[1:], jnp.bfloat16) for t in total]


def attention(qkv, w_o, cos_t, sin_t, normed_t, grad_y):
    seq, d_model = grad_y.shape
    n_steps = qkv.shape[1] // GROUP_W
    const = lambda shape: pl.BlockSpec(shape, lambda p: (0,) * len(shape), pipeline_mode=pl.Buffered(1))
    col = lambda width: pl.BlockSpec((seq, width), lambda p: (0, p))
    of_pair = lambda at: pl.BlockSpec((seq, LANES), lambda p: (0, p // 2 * (PAIR_W // LANES) + at))
    anywhere = pl.BlockSpec(memory_space=pl.ANY)
    shape = jax.ShapeDtypeStruct
    slab = pltpu.VMEM((2, seq, LANES), jnp.bfloat16)
    turned = pltpu.VMEM((HEAD, seq), jnp.bfloat16)
    acc = pltpu.VMEM((seq, LANES), jnp.float32)
    partial = [(d_model // 2, GROUP_W), (Q_COLS // 2, d_model)]
    own = [shape(p, jnp.float32) for p in partial]
    sent = [shape(p, jnp.bfloat16) for p in partial]
    totals = total_shapes(own)
    pieces = [shape((n_steps - 2,) + p.shape, p.dtype) for p in piece_shapes(totals)]
    kept = [pltpu.VMEM(p.shape, p.dtype) for p in sent + own + totals]
    out = pl.pallas_call(
        attn_kernel,
        grid=(n_steps,),
        in_specs=[pl.BlockSpec((seq, Q_COLS), lambda p: (0, p // 2 * (PAIR_W // Q_COLS) + p % 2)), of_pair(4), of_pair(5), pl.BlockSpec((Q_COLS, d_model), lambda p: (p, 0)), const((seq, LANES)), const((seq, LANES)), const((d_model, seq)), const((seq, d_model))],
        out_specs=[col(Q_COLS), col(GROUP_W)] + [anywhere] * 8,
        out_shape=[shape((seq, Q_COLS * n_steps), jnp.bfloat16), shape((seq, GROUP_W * n_steps), jnp.bfloat16)] + sent + own + totals + pieces,
        scratch_shapes=[slab, slab, slab, slab, turned, turned, pltpu.VMEM((Q_COLS, seq), jnp.bfloat16), pltpu.VMEM((Q_COLS, seq), jnp.float32), acc, acc]
        + kept + Reduce.scratch_shapes(partial) + Gather.scratch_shapes(2)
        + [pltpu.SemaphoreType.REGULAR((3,)), pltpu.SemaphoreType.DMA((6,))],
        compiler_params=pltpu.CompilerParams(vmem_limit_bytes=VMEM_LIMIT, collective_id=0, has_side_effects=True),
        cost_estimate=pl.CostEstimate(flops=COST_FLOPS, bytes_accessed=COST_BYTES, transcendentals=COST_BYTES),
        name="attn",
    )(qkv, qkv, qkv, w_o, cos_t, sin_t, normed_t, grad_y)
    return out[0], out[1], (list(out[2:4]), list(out[4:6])), list(out[6:8]), out[8:10]


def finish_kernel(o_ref, x_ref, grads_ref, gy_ref, gain_ref, wo_ref, w_hbm, sent_q, sent_d, own_q, own_d, old_q, old_d,
                  y_out, gh_out, old_pieces_q, old_pieces_d, pieces_q, pieces_d, norm_out, *scratch):
    scratch = list(scratch)
    take = lambda n: [scratch.pop(0) for _ in range(n)]
    y_s, gh_s, w_s, dh_s, norm_ref, norm_row, norm_all = take(7)
    total = take(2)
    step = pl.program_id(0)
    me = lax.axis_index('sp')
    coord, peers = axis_bits()
    reduce = Reduce(coord, peers, [sent_q, sent_d], [own_q, own_d], total, take(16))
    gather = Gather(peers, [old_q, old_d], [old_pieces_q, old_pieces_d], take(3))
    last = Gather(peers, total, [pieces_q, pieces_d], take(3))
    w_sem, y_send, y_recv, gh_send, gh_recv, norm_send, norm_recv = take(7)
    n_devs = y_out.shape[0]
    tok = y_out.shape[1]
    half_steps = pl.num_programs(0) // 2
    per_step = n_devs // half_steps
    weights = load_weights(w_hbm, w_s, w_sem, (0, GROUP_W, Q_COLS, PAIR_W - LANES))

    def share(values, out, send_sem, recv_sem, dest, act):
        @pl.when(dest == me)
        def _():
            act(pltpu.make_async_copy(values.at[dest], out.at[dest], send_sem.at[dest]), True)

        @pl.when(dest != me)
        def _():
            act(pltpu.make_async_remote_copy(src_ref=values.at[dest], dst_ref=out.at[me], send_sem=send_sem.at[dest], recv_sem=recv_sem.at[me],
                                             device_id={'sp': dest}, device_id_type=MESH), False)

    def send(values, out, send_sem, recv_sem, dests):
        for dest in dests:
            share(values, out, send_sem, recv_sem, dest, lambda copy, local: copy.start())

    def finish(values, out, send_sem, recv_sem):
        for peer in range(n_devs):
            @pl.when(peer == me)
            def _():
                pltpu.make_async_copy(values.at[peer], out.at[peer], send_sem.at[peer]).wait()

            @pl.when(peer != me)
            def _():
                pltpu.make_async_remote_copy(src_ref=values.at[peer], dst_ref=out.at[peer], send_sem=send_sem.at[peer], recv_sem=recv_sem.at[peer],
                                             device_id={'sp': peer}, device_id_type=MESH).wait()

    def share_norm(act):
        for k in range(1, n_devs):
            peer = lax.rem(me + k, n_devs)
            copy = pltpu.make_async_remote_copy(src_ref=norm_row, dst_ref=norm_all.at[me], send_sem=norm_send.at[k], recv_sem=norm_recv.at[k],
                                                device_id={'sp': peer}, device_id_type=MESH)
            act(copy)

    @pl.when(step == 0)
    def _():
        greet_all(me, n_devs)
        reduce.start()
        gather.start()
        for copy in weights:
            copy.start()
        norm_ref[...] = jnp.zeros_like(norm_ref)

    @pl.when(step == 1)
    def _():
        reduce.mid1()
        gather.mid1()

    @pl.when(jnp.logical_and(step >= 1, step <= half_steps))
    def _():
        send(y_s, y_out, y_send, y_recv, [(step - 1) * per_step + k for k in range(per_step)])

    d_model = wo_ref.shape[1]

    @pl.when(step < half_steps)
    def _():
        def cols_of_y(n, carry):
            cols = aligned(n * 512, 512)
            block = (x_ref[:, cols].astype(jnp.float32) + dot_nn(o_ref[...], wo_ref[:, cols])).astype(jnp.bfloat16)
            for k in range(per_step):
                y_s[step * per_step + k, :, cols] = block[k * tok:(k + 1) * tok, :]
            return carry
        lax.fori_loop(0, d_model // 512, cols_of_y, 0)

    @pl.when(step == half_steps)
    def _():
        for copy in weights:
            copy.wait()

        def pair_up(n, carry):
            rows = aligned(n * LANES, LANES)
            for pair in range(w_s.shape[1] // PAIR_W):
                spots = [pl.ds(pair * PAIR_W + at, LANES) for at in (Q_COLS, PAIR_W - LANES)]
                for spot, cols in zip(spots, cross(*[w_s[rows, spot].astype(jnp.float32) for spot in spots])):
                    w_s[rows, spot] = cols.astype(jnp.bfloat16)
            return carry

        lax.fori_loop(0, d_model // LANES, pair_up, 0)

    @pl.when(step >= half_steps)
    def _():
        def cols_of_dh(n, carry):
            rows = aligned(n * 512, 512)
            dh_s[:, rows] = dot_nt(grads_ref[...], w_s[rows, :])
            return carry
        lax.fori_loop(0, d_model // 512, cols_of_dh, 0)
        gain = gain_ref[...]

        def norm_rows(n, carry):
            rows = aligned(n * 16, 16)
            x_f = x_ref[rows, :].astype(jnp.float32)
            inv_rms = lax.rsqrt(jnp.mean(x_f * x_f, axis=-1, keepdims=True) + NORM_EPS)
            unit = x_f * inv_rms
            grad_normed = dh_s[rows, :]
            grad_unit = grad_normed * gain
            mean_dot = jnp.mean(grad_unit * unit, axis=-1, keepdims=True)
            grad_x = gy_ref[rows, :].astype(jnp.float32) + inv_rms * (grad_unit - unit * mean_dot)
            place = (step - half_steps) * per_step + n // (tok // 16)
            gh_s[place, aligned(lax.rem(n, tok // 16) * 16, 16), :] = grad_x.astype(jnp.bfloat16)
            weighted = grad_normed * unit
            norm_ref[...] += weighted[:8, :] + weighted[8:, :]
            return carry
        lax.fori_loop(0, per_step * tok // 16, norm_rows, 0)

    @pl.when(step == pl.num_programs(0) - 1)
    def _():
        gh = (gh_s, gh_out, gh_send, gh_recv)
        norm_row[...] = over_keys(jnp.sum, norm_ref[...])
        reduce.mid2()
        gather.mid2()
        share_norm(lambda copy: copy.start())
        send(*gh, range(n_devs // 2))
        reduce.end()
        last.start()
        send(*gh, range(n_devs // 2, n_devs))
        gather.end()
        last.mid1()
        last.mid2()
        share_norm(lambda copy: copy.wait())
        norm_all[me] = norm_row[...]
        norm_out[...] = sum(norm_all[peer] for peer in range(n_devs))
        finish(y_s, y_out, y_send, y_recv)
        last.end()
        finish(*gh)


def finish(attn, x, grads, grad_y, gain, w_o, w_qkv, reduce, old_total, n_devs):
    seq, d_model = x.shape
    sent, own = reduce
    steps = 8
    rows = 2 * seq // steps
    tok = seq // n_devs
    const = lambda shape: pl.BlockSpec(shape, lambda s: (0,) * len(shape), pipeline_mode=pl.Buffered(1))
    early = lambda width: pl.BlockSpec((rows, width), lambda s: (jnp.minimum(s, steps // 2 - 1), 0))
    late = lambda width: pl.BlockSpec((rows, width), lambda s: (jnp.maximum(s - steps // 2, 0), 0))
    anywhere = pl.BlockSpec(memory_space=pl.ANY)
    shape = jax.ShapeDtypeStruct
    totals = total_shapes(own)
    tokens = shape((n_devs, tok, d_model), jnp.bfloat16)
    dma = lambda: pltpu.SemaphoreType.DMA((n_devs,))
    out = pl.pallas_call(
        finish_kernel,
        grid=(steps,),
        in_specs=[early(q_w) for q_w in (attn.shape[1],)] + [pl.BlockSpec((rows, d_model), lambda s: (lax.rem(s, steps // 2), 0)), late(grads.shape[1]), late(d_model),
                  const((1, d_model)), const(w_o.shape), anywhere, anywhere, anywhere]
        + [const(o.shape) for o in own] + [const(t.shape) for t in totals],
        out_specs=[anywhere] * 6 + [pl.BlockSpec((1, d_model), lambda s: (0, 0))],
        out_shape=[tokens, tokens] + piece_shapes(totals) + piece_shapes(totals) + [shape((1, d_model), jnp.float32)],
        scratch_shapes=[pltpu.VMEM(tokens.shape, jnp.bfloat16), pltpu.VMEM(tokens.shape, jnp.bfloat16),
                        pltpu.VMEM(w_qkv.shape, jnp.bfloat16), pltpu.VMEM((rows, d_model), jnp.float32),
                        pltpu.VMEM((8, d_model), jnp.float32), pltpu.VMEM((1, d_model), jnp.float32),
                        pltpu.VMEM((n_devs, 1, d_model), jnp.float32)]
        + [pltpu.VMEM(t.shape, t.dtype) for t in totals]
        + Reduce.scratch_shapes([o.shape for o in own]) + Gather.scratch_shapes(2) + Gather.scratch_shapes(2)
        + [pltpu.SemaphoreType.DMA((4 * w_qkv.shape[1] // PAIR_W,))] + [dma()] * 6,
        compiler_params=pltpu.CompilerParams(vmem_limit_bytes=VMEM_LIMIT, collective_id=1, has_side_effects=True),
        cost_estimate=pl.CostEstimate(flops=COST_FLOPS, bytes_accessed=COST_BYTES, transcendentals=COST_BYTES),
        name="finish",
    )(attn, x, grads, grad_y, gain, w_o, w_qkv, *sent, *own, *old_total)
    return out[0], out[1], out[2:4], out[4:6], out[6]


def place_kernel(n, slots, *refs):
    pieces_q, pieces_d, tokens = refs[:n], refs[n:2 * n], refs[2 * n:2 * n + 2]
    q_out, d_out, *tokens_out = refs[2 * n + 2:]
    for src, dst in zip(tokens, tokens_out):
        dst[...] = src[...]
    for c in range(n):
        d_out[c] = pieces_d[c][0, 0].astype(jnp.float32)
        q_out[:, pl.ds(c * Q_COLS, Q_COLS)] = pieces_q[c][0, 0, :, :Q_COLS].astype(jnp.float32)
    for pair in range(n // 2):
        grads = cross(*[ref[0, 0, :, Q_COLS:].astype(jnp.float32) for ref in pieces_q[2 * pair:2 * pair + 2]])
        for at, grad in zip((n * Q_COLS, q_out.shape[1] - n * HEAD), grads):
            q_out[:, pl.ds(at + pair * LANES, LANES)] = grad


def place(slots, parts_q, parts_d, tokens):
    specs, args, sizes = [], [], []
    for parts in (parts_q, parts_d):
        chunks = [(part, c) for part in parts for c in range(part.shape[0])]
        rows, width = parts[0].shape[2:]
        specs += [pl.BlockSpec((1, 1, rows, width), lambda s, slots, c=c: (c, s, 0, 0)) for _, c in chunks]
        args += [part for part, _ in chunks]
        sizes.append((len(chunks), rows, width))
    (n_pairs, rows_q, width_q), (_, rows_d, width_d) = sizes
    flat = [t.reshape(16, -1, t.shape[-1]) for t in tokens]
    through = pl.BlockSpec((1,) + flat[0].shape[1:], lambda s, slots: (s, 0, 0))
    shape = jax.ShapeDtypeStruct
    grad_q, grad_d, *out = pl.pallas_call(
        functools.partial(place_kernel, n_pairs),
        grid_spec=pltpu.PrefetchScalarGridSpec(
            num_scalar_prefetch=1, grid=(16,), in_specs=specs + [through] * 2,
            out_specs=[pl.BlockSpec((rows_q, n_pairs * width_q), lambda s, slots: (slots[s], 0)),
                       pl.BlockSpec((n_pairs, rows_d, width_d), lambda s, slots: (0, slots[s], 0)), through, through]),
        out_shape=[shape((16 * rows_q, n_pairs * width_q), jnp.float32), shape((n_pairs, 16 * rows_d, width_d), jnp.float32)]
        + [shape(t.shape, t.dtype) for t in flat],
        compiler_params=pltpu.CompilerParams(vmem_limit_bytes=VMEM_LIMIT),
        cost_estimate=pl.CostEstimate(flops=COST_FLOPS, bytes_accessed=COST_BYTES, transcendentals=COST_BYTES),
        name="place",
    )(slots, *args, *flat)
    return grad_q, grad_d, [o.reshape(t.shape) for o, t in zip(out, tokens)]


def row_slots():
    me = lax.axis_index('sp')
    core, x, y = me & 1, (me >> 1) & 1, me >> 2
    order = []
    for c in (core, 1 - core):
        for half, (a, b) in enumerate(((x, y), (y, x))):
            for a_i in (a, 1 - a):
                for b_i in (b, 1 - b):
                    order.append(c * 8 + half * 4 + a_i * 2 + b_i)
    return jnp.stack(order).astype(jnp.int32)


def solution(mesh):
    n_devs = mesh.shape['sp']

    def device_step(hidden, norm_w, w_qkv, w_out, long_factor, grad_out):
        d_model = hidden.shape[-1]
        gain = norm_w.astype(jnp.float32)[None]
        x, grad_y, qkv, normed_t, cos_t, sin_t = enter(hidden, grad_out, gain, inverse_frequencies(long_factor), w_qkv)
        x, grad_y = x.reshape(-1, d_model), grad_y.reshape(-1, d_model)
        w_o = w_out.reshape(-1, d_model)
        attn, grads, partial, total, pieces = attention(qkv, w_o, cos_t, sin_t, normed_t, grad_y)
        block_out, grad_hidden, before_last, last, grad_norm_w = finish(attn, x, grads, grad_y, gain, w_o, w_qkv, partial, total, n_devs)
        parts = [[first, second[None], third[None]] for first, second, third in zip(pieces, before_last, last)]
        grad_w_qkv, grad_w_out, (block_out, grad_hidden) = place(row_slots(), *parts, (block_out, grad_hidden))
        return block_out, grad_hidden, grad_w_qkv, grad_w_out.reshape(w_out.shape), grad_norm_w.reshape(-1)

    tok_spec = P('dp', 'sp', None)
    return jax.shard_map(device_step, mesh=mesh,
                         in_specs=(tok_spec, P(), P(), P(), P(), tok_spec),
                         out_specs=(tok_spec, tok_spec, P('dp', None), P('dp', None, None), P('dp')),
                         check_vma=False)
```
